16 devices in a mesh: rep: 2 (over y, z), dp: 8 (over x, core).
Axes of the slice: x: 4, y: 2, z: 1, core: 2. Of those that a mesh axis runs over, the one named last changes fastest.
The devices are a block of a 4x4x8 slice.
Arguments:
- x: bfloat16 [16, 2048, 512], P(('rep', 'dp')), parts along dimension 0
- dy: bfloat16 [16, 2048, 512], P(('rep', 'dp')), parts along dimension 0
- w_gate: bfloat16 [2, 512, 2048], replicated
- w_up: bfloat16 [2, 512, 2048], replicated
- w_down: bfloat16 [2, 2048, 512], replicated
- m_w_gate: float32 [2, 512, 2048], replicated
- m_w_up: float32 [2, 512, 2048], replicated
- m_w_down: float32 [2, 2048, 512], replicated
- v_w_gate: float32 [2, 512, 2048], replicated
- v_w_up: float32 [2, 512, 2048], replicated
- v_w_down: float32 [2, 2048, 512], replicated
Outputs:
- output 1: bfloat16 [4, 512, 2048], P('rep'), parts along dimension 0
- output 2: bfloat16 [4, 512, 2048], P('rep'), parts along dimension 0
- output 3: bfloat16 [4, 2048, 512], P('rep'), parts along dimension 0
- output 4: float32 [4, 512, 2048], P('rep'), parts along dimension 0
- output 5: float32 [4, 512, 2048], P('rep'), parts along dimension 0
- output 6: float32 [4, 2048, 512], P('rep'), parts along dimension 0
- output 7: float32 [4, 512, 2048], P('rep'), parts along dimension 0
- output 8: float32 [4, 512, 2048], P('rep'), parts along dimension 0
- output 9: float32 [4, 2048, 512], P('rep'), parts along dimension 0
There are 2 independent parts. The reference program is written for one: setup_inputs(seed, part) draws one part's arguments, and reference() takes and returns one part's arrays. A program takes and returns all parts, laid end to end along the dimension named above; an argument that names none is the same for every part.
All inputs are finite; a program needn't handle non-finite values.
Results may differ from the reference program's by a relative error of at most 0.02.
Values are sent between devices in bfloat16 or wider.
A program may use at most 768 MiB of HBM per device.

```python
import jax
import jax.numpy as jnp
from jax import lax

SEQUENCES = 8
TOKENS = 2048
D = 512
FF = 2048
LAYERS = 2
NAMES = ("w_gate", "w_up", "w_down")
SHAPES = {"w_gate": (LAYERS, D, FF), "w_up": (LAYERS, D, FF), "w_down": (LAYERS, FF, D)}


def bump(key, n, height):
    away = (jnp.arange(n, dtype=jnp.int32) - jax.random.randint(key, (), 0, n, jnp.int32)) % n
    return jnp.where(away < n // 8, height, 1.0)


def together(key, own, strength):
    shared = jax.random.normal(key, own.shape[1:], jnp.float32)
    return (own + strength * shared) * lax.rsqrt(1 + strength * strength)


def setup_inputs(seed: int = 0, part: int = 0) -> dict:
    kx, kdy, ka, kb, kz, kf, kh, kl, *keys = jax.random.split(jax.random.key(seed), 8 + 3 * len(NAMES))
    kx, kdy, ka, kb = (jax.random.fold_in(k, part) for k in (kx, kdy, ka, kb))
    kw, km, kv = (keys[i::3] for i in range(3))
    shape = (SEQUENCES, TOKENS, D)
    much_x, much_dy = jax.random.uniform(kz, (2,), jnp.float32, 0.0, 1.0)
    loud = 2.0 ** jax.random.uniform(jax.random.fold_in(kz, 1), (), jnp.float32, -1.0, 2.0)
    layers = 2.0 ** jax.random.uniform(kl, (LAYERS, 1, 1), jnp.float32, -1.0, 1.0)
    x = together(ka, jax.random.normal(kx, shape, jnp.float32), much_x) * bump(kf, D, 4.0)
    dy = together(kb, jax.random.normal(kdy, shape, jnp.float32), much_dy)
    drawn = {"x": x.astype(jnp.bfloat16), "dy": (loud * dy * (SEQUENCES * TOKENS) ** -0.5).astype(jnp.bfloat16)}
    for key, name in zip(kw, NAMES, strict=True):
        w = jax.random.normal(key, SHAPES[name], jnp.float32) * SHAPES[name][1] ** -0.5
        drawn[name] = (w * {"w_gate": 1.0, "w_up": bump(kh, FF, 4.0), "w_down": layers}[name]).astype(jnp.bfloat16)
    for key, name in zip(km, NAMES, strict=True):
        drawn[f"m_{name}"] = 0.1 * jax.random.normal(key, SHAPES[name], jnp.float32)
    for key, name in zip(kv, NAMES, strict=True):
        drawn[f"v_{name}"] = jax.random.uniform(key, SHAPES[name], jnp.float32, 0.005, 0.015)
    return drawn


def matmul(a, w):
    return jnp.dot(a, w, preferred_element_type=jnp.float32).astype(jnp.bfloat16)


def normed(h):
    wide = h.astype(jnp.float32)
    scale = lax.rsqrt(jnp.mean(wide**2, -1, keepdims=True) + 1e-6)
    return (wide * scale).astype(jnp.bfloat16)


def layer(h, w):
    a = normed(h)
    gate = jnp.dot(a, w["w_gate"], preferred_element_type=jnp.float32)
    up = jnp.dot(a, w["w_up"], preferred_element_type=jnp.float32)
    return h + matmul((jax.nn.silu(gate) * up).astype(jnp.bfloat16), w["w_down"])


def adamw(w, m, v, g):
    m = 0.9 * m + 0.1 * g
    v = 0.95 * v + 0.05 * g * g
    step = m * lax.rsqrt(v + 1e-8) + 0.1 * w
    return (w - 0.02 * step).astype(jnp.bfloat16), m, v


def stack(weights, h):
    return lax.scan(lambda h, w: (layer(h, w), None), h, weights)[0]


def reference(x, dy, w_gate, w_up, w_down, m_w_gate, m_w_up, m_w_down, v_w_gate, v_w_up, v_w_down):
    weights = dict(zip(NAMES, (w_gate, w_up, w_down), strict=True))

    def take(so_far, sequence):
        h, by_y = sequence
        _, back = jax.vjp(lambda w: stack(w, h), weights)
        return jax.tree.map(lambda total, term: total + term.astype(jnp.float32), so_far, back(by_y)[0]), None

    none_yet = {name: jnp.zeros(w.shape, jnp.float32) for name, w in weights.items()}
    by_weights, _ = lax.scan(take, none_yet, (x, dy))
    gradients = [by_weights[name].astype(jnp.bfloat16).astype(jnp.float32) for name in NAMES]
    new = [
        adamw(w.astype(jnp.float32), m, v, g)
        for w, m, v, g in zip((w_gate, w_up, w_down), (m_w_gate, m_w_up, m_w_down), (v_w_gate, v_w_up, v_w_down), gradients, strict=True)
    ]
    return tuple(one[which] for which in range(3) for one in new)
```

```python
import functools

import jax
import jax.numpy as jnp
from jax import lax
from jax.experimental import pallas as pl
from jax.experimental.pallas import tpu as pltpu
from jax.sharding import PartitionSpec as P

BF, F32 = jnp.bfloat16, jnp.float32
MESH = pl.DeviceIdType.MESH
VMEM_LIMIT = 64 * 1024 * 1024 - 256 * 1024


def dot(a, b):
    return lax.dot_general(a, b, (((1,), (0,)), ((), ())), preferred_element_type=F32)


def dot_t(a, b):
    return lax.dot_general(a, b, (((1,), (1,)), ((), ())), preferred_element_type=F32)


def norm(h):
    wide = h.astype(F32)
    scale = lax.rsqrt(jnp.mean(wide * wide, -1, keepdims=True) + 1e-6)
    return wide, scale, (wide * scale).astype(BF)


def chain_kernel(chunk, x_ref, dy_ref, wg, wu, wd, wide_out, turned, t1, t2):
    p2, dg2, du2, p1, dg1, du1 = (wide_out.at[i] for i in range(6))
    dyt, a2t, dh1t, a1t = (turned.at[i] for i in range(4))
    d = x_ref.shape[-1]
    chunks = wg.shape[-1] // chunk
    x = x_ref[...]
    _, _, a1 = norm(x)
    a1t[...] = a1.T
    down = None
    for c in range(chunks):
        cols = pl.ds(c * chunk, chunk)
        g = dot(a1, wg[0, :, cols])
        u = dot(a1, wu[0, :, cols])
        s = jax.nn.sigmoid(g)
        silu = g * s
        p = (silu * u).astype(BF)
        p1[c] = p
        t1[c] = silu
        t2[c] = u * (s * (1.0 + g * (1.0 - s)))
        term = dot(p, wd[0, cols, :])
        down = term if down is None else down + term
    h1 = x + down.astype(BF)
    wide, scale, a2 = norm(h1)
    a2t[...] = a2.T
    dy = dy_ref[...]
    dyt[...] = dy.T
    dag = dau = None
    for c in range(chunks):
        cols = pl.ds(c * chunk, chunk)
        g = dot(a2, wg[1, :, cols])
        u = dot(a2, wu[1, :, cols])
        dp = dot_t(dy, wd[1, cols, :]).astype(BF).astype(F32)
        s = jax.nn.sigmoid(g)
        silu = g * s
        p2[c] = (silu * u).astype(BF)
        du = (dp * silu).astype(BF)
        dg = (dp * (u * (s * (1.0 + g * (1.0 - s))))).astype(BF)
        du2[c] = du
        dg2[c] = dg
        tg = dot_t(dg, wg[1, :, cols])
        tu = dot_t(du, wu[1, :, cols])
        dag = tg if dag is None else dag + tg
        dau = tu if dau is None else dau + tu
    da = (dag.astype(BF) + dau.astype(BF)).astype(F32)
    dscale = jnp.sum(da * wide, -1, keepdims=True)
    dwide = da * scale - wide * (scale * scale * scale * dscale * (1.0 / d))
    dh1 = dy + dwide.astype(BF)
    dh1t[...] = dh1.T
    for c in range(chunks):
        cols = pl.ds(c * chunk, chunk)
        dp = dot_t(dh1, wd[0, cols, :]).astype(BF).astype(F32)
        du1[c] = (dp * t1[c]).astype(BF)
        dg1[c] = (dp * t2[c]).astype(BF)


def chain(x, dy, wg, wu, wd, tile=512, chunk=512):
    tokens, d = x.shape
    ff = wg.shape[-1]
    whole = lambda w: pl.BlockSpec(w.shape, lambda i: (0, 0, 0), pipeline_mode=pl.Buffered(1))
    rows = pl.BlockSpec((tile, d), lambda i: (i, 0))
    return pl.pallas_call(
        functools.partial(chain_kernel, chunk),
        name="chain",
        grid=(tokens // tile,),
        in_specs=[rows, rows, whole(wg), whole(wu), whole(wd)],
        out_specs=[
            pl.BlockSpec((6, ff // chunk, tile, chunk), lambda i: (0, 0, i, 0)),
            pl.BlockSpec((4, d, tile), lambda i: (0, 0, i)),
        ],
        out_shape=[jax.ShapeDtypeStruct((6, ff // chunk, tokens, chunk), BF), jax.ShapeDtypeStruct((4, d, tokens), BF)],
        scratch_shapes=[pltpu.VMEM((ff // chunk, tile, chunk), F32)] * 2,
        compiler_params=pltpu.CompilerParams(dimension_semantics=("arbitrary",), vmem_limit_bytes=VMEM_LIMIT),
    )(x, dy, wg, wu, wd)


def sum_kernel(n, wide, turned, out, g_ref, d_ref, i_ref, q_ref, go, left_op, right_op, *sems):
    (op_sem, out_sem, d_s, d_r, i_s, i_r, ii_s, ii_r, iii_s, iii_r, ag1_s, ag1_r, ag2_s, ag2_r, p_s, p_r) = sems
    mats, chunks = wide.shape[:2]
    pieces = g_ref.shape[1]
    half = pieces // 2
    per = pieces // chunks
    lanes = g_ref.shape[-1]
    me = lax.axis_index("dp")
    core = lax.rem(me, 2)
    chip = me // 2
    chips = n // 2
    partner = me + 1 - 2 * core
    chip_r = lax.rem(chip + 1, chips)
    chip_l = lax.rem(chip + chips - 1, chips)
    chip_o = lax.rem(chip + 2, chips)
    toward = (chip_r, chip_l)
    behind = (chip_l, chip_r)
    device = tuple(2 * c + core for c in toward)

    def piece(c, h):
        return core * half + 2 * c + h

    def remote(src, dst, s, r, to):
        return pltpu.make_async_remote_copy(src, dst, s, r, device_id={"dp": to}, device_id_type=MESH)

    def d_copy(k):
        return remote(g_ref.at[k, pl.ds((1 - core) * half, half)], d_ref.at[k], d_s.at[k], d_r.at[k], partner)

    def i_copy(k, e):
        return remote(g_ref.at[k, piece(chip_o, e)], i_ref.at[k, e], i_s.at[k, e], i_r.at[k, e], device[e])

    def ii_copy(k, e):
        return remote(g_ref.at[k, piece(toward[e], 1 - e)], q_ref.at[k, e, 1 - e], ii_s.at[k, e], ii_r.at[k, e], device[e])

    def iii_copy(k, e):
        return remote(i_ref.at[k, e], q_ref.at[k, e, e], iii_s.at[k, e], iii_r.at[k, e], device[e])

    def ag1_copy(k, e, c):
        span = go.at[k, pl.ds(piece(c, 0), 2)]
        return remote(span, span, ag1_s.at[k, e], ag1_r.at[k, e], device[e])

    def ag2_copy(k, e, c):
        span = go.at[k, piece(c, e)]
        return remote(span, span, ag2_s.at[k, e], ag2_r.at[k, e], device[e])

    def p_copy(k, j, c, owner):
        span = go.at[k, pl.ds(owner * half + 2 * c, 2)]
        return remote(span, span, p_s.at[k, j], p_r.at[k, j], partner)

    def left_load(k, slot):
        return pltpu.make_async_copy(turned.at[(2 * k + 1) // 3], left_op.at[slot], op_sem.at[slot])

    def right_load(t):
        k, c = t // chunks, lax.rem(t, chunks)
        c = lax.rem(c + (1 - core) * (chunks // 2), chunks)
        return pltpu.make_async_copy(wide.at[k, c], right_op.at[lax.rem(t, 3)], op_sem.at[2 + lax.rem(t, 3)])

    barrier = pltpu.get_barrier_semaphore()
    for to in (*device, partner):
        pl.semaphore_signal(barrier, inc=1, device_id={"dp": to}, device_id_type=MESH)
    left_load(0, 0).start()
    right_load(0).start()
    right_load(1).start()
    pl.semaphore_wait(barrier, 3)

    def multiply(k, c):
        t = k * chunks + c
        right_load(t).wait()

        @pl.when(t + 2 < mats * chunks)
        def _():
            right_load(t + 2).start()

        where = lax.rem(c + (1 - core) * (chunks // 2), chunks) * per
        a = left_op[lax.rem(k, 2)]
        for j in range(0, per, 2):
            b = right_op[lax.rem(t, 3), :, j * lanes : (j + 2) * lanes]
            block = dot(a, b).astype(BF)
            g_ref[k, where + j] = block[:, :lanes]
            g_ref[k, where + j + 1] = block[:, lanes:]

    def reduce_1(k):
        d_copy(k).wait_recv()
        for c in (chip_o, chip_r, chip_l, chip):
            for h in range(2):
                one = g_ref[k, piece(c, h)].astype(F32) + d_ref[k, 2 * c + h].astype(F32)
                g_ref[k, piece(c, h)] = one.astype(BF)
        for e in range(2):
            i_copy(k, e).start()
        for e in range(2):
            ii_copy(k, e).start()

    def reduce_2(k):
        for e in range(2):
            i_copy(k, e).wait_recv()
            one = g_ref[k, piece(toward[e], e)].astype(F32) + i_ref[k, e].astype(F32)
            i_ref[k, e] = one.astype(BF)
            iii_copy(k, e).start()

    def reduce_3(k):
        for e in range(2):
            ii_copy(k, e).wait_recv()
            iii_copy(k, e).wait_recv()
        for h in range(2):
            one = g_ref[k, piece(chip, h)].astype(F32) + q_ref[k, 0, h].astype(F32) + q_ref[k, 1, h].astype(F32)
            go[k, piece(chip, h)] = one.astype(BF)
        for e in range(2):
            ag1_copy(k, e, chip).start()
        p_copy(k, 0, chip, core).start()

    def gather_2(k):
        for e in range(2):
            ag1_copy(k, e, behind[e]).wait_recv()
            ag2_copy(k, e, behind[e]).start()
            p_copy(k, 1 + e, behind[e], core).start()

    def gather_3(k):
        for e in range(2):
            ag2_copy(k, e, chip_o).wait_recv()
        p_copy(k, 3, chip_o, core).start()

    def done_copy(k):
        return pltpu.make_async_copy(go.at[k], out.at[k], out_sem.at[k])

    def finish(k):
        for j, c in enumerate((chip, *behind, chip_o)):
            p_copy(k, j, c, 1 - core).wait_recv()
        done_copy(k).start()

    def when(condition):
        return pl.when(condition)

    def step(k, carry):
        @when(k < mats)
        def _():
            left_load(k, lax.rem(k, 2)).wait()

            @when(k + 1 < mats)
            def _():
                left_load(k + 1, lax.rem(k + 1, 2)).start()

            lax.fori_loop(0, chunks // 2, lambda c, _: multiply(k, c), None)
            d_copy(k).start()

        @when(k >= 1)
        def _():
            reduce_2(k - 1)

        @when(k < mats)
        def _():
            lax.fori_loop(chunks // 2, chunks, lambda c, _: multiply(k, c), None)
            reduce_1(k)

        @when(k >= 3)
        def _():
            gather_2(k - 3)

        @when(k >= 1)
        def _():
            reduce_3(k - 1)

        return carry

    lax.fori_loop(0, mats + 1, step, 0)
    lax.fori_loop(mats - 2, mats, lambda k, _: gather_2(k), None)
    lax.fori_loop(0, mats, lambda k, _: gather_3(k), None)
    lax.fori_loop(0, mats, lambda k, _: finish(k), None)

    def drain(k, carry):
        d_copy(k).wait_send()
        for e in range(2):
            i_copy(k, e).wait_send()
            ii_copy(k, e).wait_send()
            iii_copy(k, e).wait_send()
            ag1_copy(k, e, chip).wait_send()
            ag2_copy(k, e, behind[e]).wait_send()
        for j, c in enumerate((chip, *behind, chip_o)):
            p_copy(k, j, c, core).wait_send()
        done_copy(k).wait()
        return carry

    lax.fori_loop(0, mats, drain, 0)


def gradients(wide, turned, n):
    mats, chunks, tokens, chunk = wide.shape
    d = turned.shape[1]
    pieces = 2 * n
    lanes = chunks * chunk // pieces
    dma = lambda *shape: pltpu.SemaphoreType.DMA(shape)
    pairs = [dma(mats), dma(mats)] + [dma(mats, 2)] * 10 + [dma(mats, 4)] * 2
    return pl.pallas_call(
        functools.partial(sum_kernel, n),
        name="gradients",
        in_specs=[pl.BlockSpec(memory_space=pl.ANY)] * 2,
        out_specs=pl.BlockSpec(memory_space=pl.ANY),
        out_shape=jax.ShapeDtypeStruct((mats, pieces, d, lanes), BF),
        scratch_shapes=[
            pltpu.VMEM((mats, pieces, d, lanes), BF),
            pltpu.VMEM((mats, pieces // 2, d, lanes), BF),
            pltpu.VMEM((mats, 2, d, lanes), BF),
            pltpu.VMEM((mats, 2, 2, d, lanes), BF),
            pltpu.VMEM((mats, pieces, d, lanes), BF),
            pltpu.VMEM((2, d, tokens), BF),
            pltpu.VMEM((3, tokens, chunk), BF),
            dma(5),
            dma(mats),
            *pairs,
        ],
        compiler_params=pltpu.CompilerParams(collective_id=0, has_side_effects=True, vmem_limit_bytes=VMEM_LIMIT),
    )(wide, turned)


def adamw(w, m, v, g):
    m = 0.9 * m + 0.1 * g
    v = 0.95 * v + 0.05 * g * g
    step = m * lax.rsqrt(v + 1e-8) + 0.1 * w
    return (w - 0.02 * step).astype(BF), m, v


def update_kernel(blocks, g_ref, *refs):
    ins, outs = refs[:9], refs[9:]
    t = pl.program_id(0)
    count, lanes = g_ref.shape[1], g_ref.shape[-1]
    for a in range(3):

        @pl.when(t // blocks == a)
        def _():
            w, m, v = (ins[a + 3 * i] for i in range(3))
            for j in range(count):
                span = pl.ds(j * lanes, lanes)
                g = g_ref[0, j].astype(F32)
                if a == 2:
                    at = (0, span, slice(None))
                    g = g.T
                else:
                    at = (0, slice(None), span)
                nw, nm, nv = adamw(w[at].astype(F32), m[at], v[at], g)
                outs[a][at] = nw
                outs[a + 3][at] = nm
                outs[a + 6][at] = nv


def update(g, weights, m, v, per_layer=4):
    layers, d, ff = weights[0].shape
    blocks = layers * per_layer
    count = g.shape[1] // per_layer
    order = (1, 2, 0)

    def g_map(t):
        a, b = t // blocks, lax.rem(t, blocks)
        return (layers - 1 - b // per_layer) * 3 + lax.rem(a + 1, 3), lax.rem(b, per_layer), 0, 0

    def spec(a):
        def at(t):
            b = jnp.clip(t - a * blocks, 0, blocks - 1)
            layer, part = b // per_layer, lax.rem(b, per_layer)
            return (layer, part, 0) if a == 2 else (layer, 0, part)

        return pl.BlockSpec((1, ff // per_layer, d) if a == 2 else (1, d, ff // per_layer), at)

    specs = [spec(a) for a in range(3)] * 3
    arrays = (*weights, *m, *v)
    return pl.pallas_call(
        functools.partial(update_kernel, blocks),
        name="update",
        grid=(3 * blocks,),
        in_specs=[pl.BlockSpec((1, count, *g.shape[2:]), g_map), *specs],
        out_specs=specs,
        out_shape=[jax.ShapeDtypeStruct(x.shape, x.dtype) for x in arrays],
        compiler_params=pltpu.CompilerParams(dimension_semantics=("arbitrary",), vmem_limit_bytes=VMEM_LIMIT),
    )(g, *arrays)


def solution(mesh):
    n = mesh.shape["dp"]

    def step(x, dy, *arrays):
        weights, m, v = (arrays[i : i + 3] for i in (0, 3, 6))
        wide, turned = chain(x[0], dy[0], *weights)
        g = gradients(wide, turned, n)
        return tuple(update(g, weights, m, v))

    return jax.shard_map(
        step,
        mesh=mesh,
        in_specs=(P(("rep", "dp"), None, None),) * 2 + (P(None, None, None),) * 9,
        out_specs=(P("rep", None, None),) * 9,
        check_vma=False,
    )
```

```python
import functools

import jax
import jax.numpy as jnp
import numpy as np
from jax import lax
from jax.experimental import pallas as pl
from jax.experimental.pallas import tpu as pltpu
from jax.sharding import PartitionSpec as P

BF, F32 = jnp.bfloat16, jnp.float32
MESH = pl.DeviceIdType.MESH
VMEM_LIMIT = 64 * 1024 * 1024 - 256 * 1024


def dot(a, b):
    return lax.dot_general(a, b, (((1,), (0,)), ((), ())), preferred_element_type=F32)


def dot_t(a, b):
    return lax.dot_general(a, b, (((1,), (1,)), ((), ())), preferred_element_type=F32)


def norm(h):
    wide = h.astype(F32)
    scale = lax.rsqrt(jnp.mean(wide * wide, -1, keepdims=True) + 1e-6)
    return wide, scale, (wide * scale).astype(BF)


def chain_kernel(chunk, x_ref, dy_ref, wg, wu, wd, wide_out, turned, t1, t2):
    p2, dg2, du2, p1, dg1, du1 = (wide_out.at[i] for i in range(6))
    dyt, a2t, dh1t, a1t = (turned.at[i] for i in range(4))
    d = x_ref.shape[-1]
    chunks = wg.shape[-1] // chunk
    x = x_ref[...]
    _, _, a1 = norm(x)
    a1t[...] = a1.T
    down = None
    for c in range(chunks):
        cols = pl.ds(c * chunk, chunk)
        g = dot(a1, wg[0, :, cols])
        u = dot(a1, wu[0, :, cols])
        s = jax.nn.sigmoid(g)
        silu = g * s
        p = (silu * u).astype(BF)
        p1[c] = p
        t1[c] = silu
        t2[c] = u * (s * (1.0 + g * (1.0 - s)))
        term = dot(p, wd[0, cols, :])
        down = term if down is None else down + term
    h1 = x + down.astype(BF)
    wide, scale, a2 = norm(h1)
    a2t[...] = a2.T
    dy = dy_ref[...]
    dyt[...] = dy.T
    dag = dau = None
    for c in range(chunks):
        cols = pl.ds(c * chunk, chunk)
        g = dot(a2, wg[1, :, cols])
        u = dot(a2, wu[1, :, cols])
        dp = dot_t(dy, wd[1, cols, :]).astype(BF).astype(F32)
        s = jax.nn.sigmoid(g)
        silu = g * s
        p2[c] = (silu * u).astype(BF)
        du = (dp * silu).astype(BF)
        dg = (dp * (u * (s * (1.0 + g * (1.0 - s))))).astype(BF)
        du2[c] = du
        dg2[c] = dg
        tg = dot_t(dg, wg[1, :, cols])
        tu = dot_t(du, wu[1, :, cols])
        dag = tg if dag is None else dag + tg
        dau = tu if dau is None else dau + tu
    da = (dag.astype(BF) + dau.astype(BF)).astype(F32)
    dscale = jnp.sum(da * wide, -1, keepdims=True)
    dwide = da * scale - wide * (scale * scale * scale * dscale * (1.0 / d))
    dh1 = dy + dwide.astype(BF)
    dh1t[...] = dh1.T
    for c in range(chunks):
        cols = pl.ds(c * chunk, chunk)
        dp = dot_t(dh1, wd[0, cols, :]).astype(BF).astype(F32)
        du1[c] = (dp * t1[c]).astype(BF)
        dg1[c] = (dp * t2[c]).astype(BF)


def chain(x, dy, wg, wu, wd, tile=512, chunk=512):
    tokens, d = x.shape
    ff = wg.shape[-1]
    whole = lambda w: pl.BlockSpec(w.shape, lambda i: (0, 0, 0), pipeline_mode=pl.Buffered(1))
    rows = pl.BlockSpec((tile, d), lambda i: (i, 0))
    return pl.pallas_call(
        functools.partial(chain_kernel, chunk),
        name="chain",
        grid=(tokens // tile,),
        in_specs=[rows, rows, whole(wg), whole(wu), whole(wd)],
        out_specs=[
            pl.BlockSpec((6, ff // chunk, tile, chunk), lambda i: (0, 0, i, 0)),
            pl.BlockSpec((4, d, tile), lambda i: (0, 0, i)),
        ],
        out_shape=[jax.ShapeDtypeStruct((6, ff // chunk, tokens, chunk), BF), jax.ShapeDtypeStruct((4, d, tokens), BF)],
        scratch_shapes=[pltpu.VMEM((ff // chunk, tile, chunk), F32)] * 2,
        compiler_params=pltpu.CompilerParams(dimension_semantics=("arbitrary",), vmem_limit_bytes=VMEM_LIMIT),
    )(x, dy, wg, wu, wd)


def sum_kernel(n, wide, turned, out, shard_a, shard_b, g_ref, d_ref, i_ref, q_ref, go, own, left_op, right_op, *sems):
    (op_sem, out_sem, own_sem, d_s, d_r, i_s, i_r, ii_s, ii_r, iii_s, iii_r, ag1_s, ag1_r, ag2_s, ag2_r, p_s, p_r) = sems
    mats, chunks = wide.shape[:2]
    early = go.shape[0]
    shards = (shard_a, shard_b)
    pieces = g_ref.shape[1]
    half = pieces // 2
    per = pieces // chunks
    lanes = g_ref.shape[-1]
    me = lax.axis_index("dp")
    core = lax.rem(me, 2)
    chip = me // 2
    chips = n // 2
    partner = me + 1 - 2 * core
    chip_r = lax.rem(chip + 1, chips)
    chip_l = lax.rem(chip + chips - 1, chips)
    chip_o = lax.rem(chip + 2, chips)
    toward = (chip_r, chip_l)
    behind = (chip_l, chip_r)
    device = tuple(2 * c + core for c in toward)

    def piece(c, h):
        return core * half + 2 * c + h

    def remote(src, dst, s, r, to):
        return pltpu.make_async_remote_copy(src, dst, s, r, device_id={"dp": to}, device_id_type=MESH)

    def d_copy(k):
        return remote(g_ref.at[k, pl.ds((1 - core) * half, half)], d_ref.at[k], d_s.at[k], d_r.at[k], partner)

    def i_copy(k, e):
        return remote(g_ref.at[k, piece(chip_o, e)], i_ref.at[k, e], i_s.at[k, e], i_r.at[k, e], device[e])

    def ii_copy(k, e):
        return remote(g_ref.at[k, piece(toward[e], 1 - e)], q_ref.at[k, e, 1 - e], ii_s.at[k, e], ii_r.at[k, e], device[e])

    def iii_copy(k, e):
        return remote(i_ref.at[k, e], q_ref.at[k, e, e], iii_s.at[k, e], iii_r.at[k, e], device[e])

    def ag1_copy(k, e, c):
        span = go.at[k, pl.ds(piece(c, 0), 2)]
        return remote(span, span, ag1_s.at[k, e], ag1_r.at[k, e], device[e])

    def ag2_copy(k, e, c):
        span = go.at[k, piece(c, e)]
        return remote(span, span, ag2_s.at[k, e], ag2_r.at[k, e], device[e])

    def p_copy(k, j, c, owner):
        span = go.at[k, pl.ds(owner * half + 2 * c, 2)]
        return remote(span, span, p_s.at[k, j], p_r.at[k, j], partner)

    def left_load(k, slot):
        return pltpu.make_async_copy(turned.at[(2 * k + 1) // 3], left_op.at[slot], op_sem.at[slot])

    def right_load(t):
        k, c = t // chunks, lax.rem(t, chunks)
        c = lax.rem(c + (1 - core) * (chunks // 2), chunks)
        return pltpu.make_async_copy(wide.at[k, c], right_op.at[lax.rem(t, 3)], op_sem.at[2 + lax.rem(t, 3)])

    barrier = pltpu.get_barrier_semaphore()
    for to in (*device, partner):
        pl.semaphore_signal(barrier, inc=1, device_id={"dp": to}, device_id_type=MESH)
    left_load(0, 0).start()
    right_load(0).start()
    right_load(1).start()
    pl.semaphore_wait(barrier, 3)

    def multiply(k, c):
        t = k * chunks + c
        right_load(t).wait()

        @pl.when(t + 2 < mats * chunks)
        def _():
            right_load(t + 2).start()

        where = lax.rem(c + (1 - core) * (chunks // 2), chunks) * per
        a = left_op[lax.rem(k, 2)]
        for j in range(0, per, 2):
            b = right_op[lax.rem(t, 3), :, j * lanes : (j + 2) * lanes]
            block = dot(a, b).astype(BF)
            g_ref[k, where + j] = block[:, :lanes]
            g_ref[k, where + j + 1] = block[:, lanes:]

    def reduce_1(k):
        d_copy(k).wait_recv()
        for c in (chip_o, chip_r, chip_l, chip):
            for h in range(2):
                one = g_ref[k, piece(c, h)].astype(F32) + d_ref[k, 2 * c + h].astype(F32)
                g_ref[k, piece(c, h)] = one.astype(BF)
        for e in range(2):
            i_copy(k, e).start()
        for e in range(2):
            ii_copy(k, e).start()

    def reduce_2(k):
        for e in range(2):
            i_copy(k, e).wait_recv()
            one = g_ref[k, piece(toward[e], e)].astype(F32) + i_ref[k, e].astype(F32)
            i_ref[k, e] = one.astype(BF)
            iii_copy(k, e).start()

    def reduce_3(k):
        for e in range(2):
            ii_copy(k, e).wait_recv()
            iii_copy(k, e).wait_recv()

        def total(h):
            one = g_ref[k, piece(chip, h)].astype(F32) + q_ref[k, 0, h].astype(F32) + q_ref[k, 1, h].astype(F32)
            return one.astype(BF)

        @pl.when(k < early)
        def _():
            for h in range(2):
                go[k, piece(chip, h)] = total(h)
            for e in range(2):
                ag1_copy(k, e, chip).start()
            p_copy(k, 0, chip, core).start()

        @pl.when(k >= early)
        def _():
            for h in range(2):
                own[h, k - early] = total(h)
            for h in range(2):
                own_copy(k - early, h).start()

    def own_copy(k, h):
        return pltpu.make_async_copy(own.at[h, k], shards[h].at[k], own_sem.at[k, h])

    def gather_2(k):
        for e in range(2):
            ag1_copy(k, e, behind[e]).wait_recv()
            ag2_copy(k, e, behind[e]).start()
            p_copy(k, 1 + e, behind[e], core).start()

    def gather_3(k):
        for e in range(2):
            ag2_copy(k, e, chip_o).wait_recv()
        p_copy(k, 3, chip_o, core).start()

    def done_copy(k):
        return pltpu.make_async_copy(go.at[k], out.at[k], out_sem.at[k])

    def finish(k):
        for j, c in enumerate((chip, *behind, chip_o)):
            p_copy(k, j, c, 1 - core).wait_recv()
        done_copy(k).start()

    def when(condition):
        return pl.when(condition)

    def step(k, carry):
        @when(k < mats)
        def _():
            left_load(k, lax.rem(k, 2)).wait()

            @when(k + 1 < mats)
            def _():
                left_load(k + 1, lax.rem(k + 1, 2)).start()

            lax.fori_loop(0, chunks // 2, lambda c, _: multiply(k, c), None)
            d_copy(k).start()

        @when(k >= 1)
        def _():
            reduce_2(k - 1)

        @when(k < mats)
        def _():
            lax.fori_loop(chunks // 2, chunks, lambda c, _: multiply(k, c), None)
            reduce_1(k)

        @when(k >= mats + 1 - early)
        def _():
            gather_2(k - (mats + 1 - early))

        @when(k >= 1)
        def _():
            reduce_3(k - 1)

        return carry

    lax.fori_loop(0, mats + 1, step, 0)
    lax.fori_loop(0, early, lambda k, _: gather_3(k), None)
    lax.fori_loop(0, early, lambda k, _: finish(k), None)

    def drain(k, carry):
        d_copy(k).wait_send()
        for e in range(2):
            i_copy(k, e).wait_send()
            ii_copy(k, e).wait_send()
            iii_copy(k, e).wait_send()
        return carry

    def drain_early(k, carry):
        for e in range(2):
            ag1_copy(k, e, chip).wait_send()
            ag2_copy(k, e, behind[e]).wait_send()
        for j, c in enumerate((chip, *behind, chip_o)):
            p_copy(k, j, c, core).wait_send()
        done_copy(k).wait()
        return carry

    def drain_late(k, carry):
        for h in range(2):
            own_copy(k, h).wait()
        return carry

    lax.fori_loop(0, mats, drain, 0)
    lax.fori_loop(0, early, drain_early, 0)
    lax.fori_loop(0, mats - early, drain_late, 0)


def gradients(wide, turned, n):
    mats, chunks, tokens, chunk = wide.shape
    d = turned.shape[1]
    early = late = mats // 2
    pieces = 2 * n
    lanes = chunks * chunk // pieces
    dma = lambda *shape: pltpu.SemaphoreType.DMA(shape)
    pairs = [dma(mats), dma(mats)] + [dma(mats, 2)] * 6 + [dma(early, 2)] * 4 + [dma(early, 4)] * 2
    return pl.pallas_call(
        functools.partial(sum_kernel, n),
        name="gradients",
        in_specs=[pl.BlockSpec(memory_space=pl.ANY)] * 2,
        out_specs=[pl.BlockSpec(memory_space=pl.ANY)] * 3,
        out_shape=[jax.ShapeDtypeStruct((early, pieces, d, lanes), BF)] + [jax.ShapeDtypeStruct((late, d, lanes), BF)] * 2,
        scratch_shapes=[
            pltpu.VMEM((mats, pieces, d, lanes), BF),
            pltpu.VMEM((mats, pieces // 2, d, lanes), BF),
            pltpu.VMEM((mats, 2, d, lanes), BF),
            pltpu.VMEM((mats, 2, 2, d, lanes), BF),
            pltpu.VMEM((early, pieces, d, lanes), BF),
            pltpu.VMEM((2, late, d, lanes), BF),
            pltpu.VMEM((2, d, tokens), BF),
            pltpu.VMEM((3, tokens, chunk), BF),
            dma(5),
            dma(early),
            dma(late, 2),
            *pairs,
        ],
        compiler_params=pltpu.CompilerParams(collective_id=0, has_side_effects=True, vmem_limit_bytes=VMEM_LIMIT),
    )(wide, turned)


def adamw(w, m, v, g):
    m = 0.9 * m + 0.1 * g
    v = 0.95 * v + 0.05 * g * g
    step = m * lax.rsqrt(v + 1e-8) + 0.1 * w
    return (w - 0.02 * step).astype(BF), m, v


def apply(a, ins, outs, pieces, lanes):
    w, m, v = (ins[a + 3 * i] for i in range(3))
    for j, piece in enumerate(pieces):
        span = pl.ds(j * lanes, lanes)
        g = piece.astype(F32)
        at = (0, span, slice(None)) if a == 2 else (0, slice(None), span)
        if a == 2:
            g = g.T
        new = adamw(w[at].astype(F32), m[at], v[at], g)
        for i in range(3):
            outs[a + 3 * i][at] = new[i]


def cost(elements):
    return pl.CostEstimate(flops=150 * elements, bytes_accessed=22 * elements, transcendentals=elements)


def update_whole_kernel(blocks, g_ref, *refs):
    t = pl.program_id(0)
    for a in range(3):

        @pl.when(t // blocks == a)
        def _():
            apply(a, refs[:9], refs[9:], [g_ref[0, j] for j in range(g_ref.shape[1])], g_ref.shape[-1])


def update_whole(g, layer, arrays, blocks=4):
    _, d, ff = arrays[0].shape
    count = g.shape[1] // blocks

    def spec(a):
        def at(t):
            b = jnp.clip(t - a * blocks, 0, blocks - 1)
            return (layer, b, 0) if a == 2 else (layer, 0, b)

        return pl.BlockSpec((1, ff // blocks, d) if a == 2 else (1, d, ff // blocks), at)

    specs = [spec(a) for a in range(3)] * 3
    return pl.pallas_call(
        functools.partial(update_whole_kernel, blocks),
        name="update_whole",
        grid=(3 * blocks,),
        in_specs=[pl.BlockSpec((1, count, *g.shape[2:]), lambda t: (lax.rem(t // blocks + 1, 3), lax.rem(t, blocks), 0, 0)), *specs],
        out_specs=specs,
        out_shape=[jax.ShapeDtypeStruct(x.shape, x.dtype) for x in arrays],
        cost_estimate=cost(3 * d * ff),
        compiler_params=pltpu.CompilerParams(dimension_semantics=("arbitrary",), vmem_limit_bytes=VMEM_LIMIT),
    )(g, *arrays)


def update_part_kernel(count, where, *refs):
    sources, refs = refs[: 2 * count], refs[2 * count :]
    ins, outs, held = refs[:9], refs[18:27], refs[27]
    t = pl.program_id(0)
    for s in range(count):

        @pl.when(lax.rem(t, count) == s)
        def _():
            held[0] = sources[2 * s][0]
            held[1] = sources[2 * s + 1][0]

    for a in range(3):

        @pl.when(t // count == a)
        def _():
            apply(a, ins, outs, [held[0], held[1]], held.shape[-1])


def update_part(sources, where, layer, arrays, new):
    _, d, _ = arrays[0].shape
    count = len(sources)
    lanes = sources[0][0].shape[-1]

    def spec(a):
        def at(t, where):
            b = where[jnp.clip(t - a * count, 0, count - 1)]
            return (layer, b, 0) if a == 2 else (layer, 0, b)

        return pl.BlockSpec((1, 2 * lanes, d) if a == 2 else (1, d, 2 * lanes), at)

    specs = [spec(a) for a in range(3)] * 3
    shard = pl.BlockSpec((1, d, lanes), lambda t, where: (lax.rem(t // count + 1, 3), 0, 0))
    return pl.pallas_call(
        functools.partial(update_part_kernel, count),
        name="update_part",
        grid_spec=pltpu.PrefetchScalarGridSpec(
            num_scalar_prefetch=1,
            grid=(3 * count,),
            in_specs=[shard] * (2 * count) + specs + [pl.BlockSpec(memory_space=pl.ANY)] * 9,
            out_specs=specs,
            scratch_shapes=[pltpu.VMEM((2, d, lanes), BF)],
        ),
        out_shape=[jax.ShapeDtypeStruct(x.shape, x.dtype) for x in arrays],
        input_output_aliases={1 + 2 * count + 9 + i: i for i in range(9)},
        cost_estimate=cost(3 * count * 2 * lanes * d),
        compiler_params=pltpu.CompilerParams(dimension_semantics=("arbitrary",), vmem_limit_bytes=VMEM_LIMIT),
    )(where, *[x for pair in sources for x in pair], *arrays, *new)


def solution(mesh):
    n = mesh.shape["dp"]
    to_right = [(i, (i + 2) % n) for i in range(n)]
    to_left = [(i, (i - 2) % n) for i in range(n)]
    across = [(i, i ^ 1) for i in range(n)]

    chips = n // 2
    at = lambda i, other, ahead: (i % 2 + other) % 2 * chips + (i // 2 + ahead) % chips
    steps = ((0, 0), (1, 0), (0, -1), (0, 1), (1, -1), (1, 1), (0, 2), (1, 2))
    places = np.array([[at(i, *step) for step in steps] for i in range(n)], np.int32)

    def send(pair, to):
        return tuple(lax.ppermute(x, "dp", to) for x in pair)

    def step(x, dy, *arrays):
        weights = arrays[:3]
        wide, turned = chain(x[0], dy[0], *weights)
        g, *own = gradients(wide, turned, n)
        left, right, other = send(own, to_right), send(own, to_left), send(own, across)
        new = update_whole(g, 1, arrays)
        left, right, first = lax.optimization_barrier((left, right, new[0]))
        new = [first, *new[1:]]
        far = (*send(left[:1], to_right), *send(right[1:], to_left))
        other_left, other_right = send(left, across), send(right, across)
        where = lax.dynamic_index_in_dim(jnp.asarray(places), lax.axis_index("dp"), 0, keepdims=False)
        new = update_part([own, other, left, right], where[:4], 0, arrays, new)
        far, first = lax.optimization_barrier((far, new[0]))
        new = [first, *new[1:]]
        other_far = send(far, across)
        new = update_part([other_left, other_right, far], where[4:7], 0, arrays, new)
        return tuple(update_part([other_far], where[7:], 0, arrays, new))

    return jax.shard_map(
        step,
        mesh=mesh,
        in_specs=(P(("rep", "dp"), None, None),) * 2 + (P(None, None, None),) * 9,
        out_specs=(P("rep", None, None),) * 9,
        check_vma=False,
    )
```

```python
import functools

import jax
import jax.numpy as jnp
from jax import lax
from jax.experimental import pallas as pl
from jax.experimental.pallas import tpu as pltpu
from jax.sharding import PartitionSpec as P

BF, F32 = jnp.bfloat16, jnp.float32
MESH = pl.DeviceIdType.MESH
VMEM_LIMIT = 64 * 1024 * 1024 - 256 * 1024


def dot(a, b):
    return lax.dot_general(a, b, (((1,), (0,)), ((), ())), preferred_element_type=F32)


def dot_t(a, b):
    return lax.dot_general(a, b, (((1,), (1,)), ((), ())), preferred_element_type=F32)


def norm(h):
    wide = h.astype(F32)
    scale = lax.rsqrt(jnp.mean(wide * wide, -1, keepdims=True) + 1e-6)
    return wide, scale, (wide * scale).astype(BF)


def chain_kernel(chunk, x_ref, dy_ref, wg, wu, wd, wide_out, turned, t1, t2):
    p2, dg2, du2, p1, dg1, du1 = (wide_out.at[i] for i in range(6))
    dyt, a2t, dh1t, a1t = (turned.at[i] for i in range(4))
    d = x_ref.shape[-1]
    chunks = wg.shape[-1] // chunk
    x = x_ref[...]
    _, _, a1 = norm(x)
    a1t[...] = a1.T
    down = None
    for c in range(chunks):
        cols = pl.ds(c * chunk, chunk)
        g = dot(a1, wg[0, :, cols])
        u = dot(a1, wu[0, :, cols])
        s = jax.nn.sigmoid(g)
        silu = g * s
        p = (silu * u).astype(BF)
        p1[c] = p
        t1[c] = silu
        t2[c] = u * (s * (1.0 + g * (1.0 - s)))
        term = dot(p, wd[0, cols, :])
        down = term if down is None else down + term
    h1 = x + down.astype(BF)
    wide, scale, a2 = norm(h1)
    a2t[...] = a2.T
    dy = dy_ref[...]
    dyt[...] = dy.T
    dag = dau = None
    for c in range(chunks):
        cols = pl.ds(c * chunk, chunk)
        g = dot(a2, wg[1, :, cols])
        u = dot(a2, wu[1, :, cols])
        dp = dot_t(dy, wd[1, cols, :]).astype(BF).astype(F32)
        s = jax.nn.sigmoid(g)
        silu = g * s
        p2[c] = (silu * u).astype(BF)
        du = (dp * silu).astype(BF)
        dg = (dp * (u * (s * (1.0 + g * (1.0 - s))))).astype(BF)
        du2[c] = du
        dg2[c] = dg
        tg = dot_t(dg, wg[1, :, cols])
        tu = dot_t(du, wu[1, :, cols])
        dag = tg if dag is None else dag + tg
        dau = tu if dau is None else dau + tu
    da = (dag.astype(BF) + dau.astype(BF)).astype(F32)
    dscale = jnp.sum(da * wide, -1, keepdims=True)
    dwide = da * scale - wide * (scale * scale * scale * dscale * (1.0 / d))
    dh1 = dy + dwide.astype(BF)
    dh1t[...] = dh1.T
    for c in range(chunks):
        cols = pl.ds(c * chunk, chunk)
        dp = dot_t(dh1, wd[0, cols, :]).astype(BF).astype(F32)
        du1[c] = (dp * t1[c]).astype(BF)
        dg1[c] = (dp * t2[c]).astype(BF)


def chain(x, dy, wg, wu, wd, tile=512, chunk=512):
    tokens, d = x.shape
    ff = wg.shape[-1]
    whole = lambda w: pl.BlockSpec(w.shape, lambda i: (0, 0, 0), pipeline_mode=pl.Buffered(1))
    rows = pl.BlockSpec((tile, d), lambda i: (i, 0))
    return pl.pallas_call(
        functools.partial(chain_kernel, chunk),
        name="chain",
        grid=(tokens // tile,),
        in_specs=[rows, rows, whole(wg), whole(wu), whole(wd)],
        out_specs=[
            pl.BlockSpec((6, ff // chunk, tile, chunk), lambda i: (0, 0, i, 0)),
            pl.BlockSpec((4, d, tile), lambda i: (0, 0, i)),
        ],
        out_shape=[jax.ShapeDtypeStruct((6, ff // chunk, tokens, chunk), BF), jax.ShapeDtypeStruct((4, d, tokens), BF)],
        scratch_shapes=[pltpu.VMEM((ff // chunk, tile, chunk), F32)] * 2,
        compiler_params=pltpu.CompilerParams(dimension_semantics=("arbitrary",), vmem_limit_bytes=VMEM_LIMIT),
    )(x, dy, wg, wu, wd)


def sum_kernel(n, wide, turned, out, shard_a, shard_b, g_ref, d_ref, i_ref, q_ref, go, own, left_op, right_op, *sems):
    (op_sem, out_sem, own_sem, d_s, d_r, i_s, i_r, ii_s, ii_r, iii_s, iii_r, ag1_s, ag1_r, ag2_s, ag2_r, p_s, p_r) = sems
    mats, chunks = wide.shape[:2]
    early = go.shape[0]
    shards = (shard_a, shard_b)
    pieces = g_ref.shape[1]
    half = pieces // 2
    per = pieces // chunks
    lanes = g_ref.shape[-1]
    me = lax.axis_index("dp")
    core = lax.rem(me, 2)
    chip = me // 2
    chips = n // 2
    partner = me + 1 - 2 * core
    chip_r = lax.rem(chip + 1, chips)
    chip_l = lax.rem(chip + chips - 1, chips)
    chip_o = lax.rem(chip + 2, chips)
    toward = (chip_r, chip_l)
    behind = (chip_l, chip_r)
    device = tuple(2 * c + core for c in toward)

    def piece(c, h):
        return core * half + 2 * c + h

    def remote(src, dst, s, r, to):
        return pltpu.make_async_remote_copy(src, dst, s, r, device_id={"dp": to}, device_id_type=MESH)

    def d_copy(k):
        return remote(g_ref.at[k, pl.ds((1 - core) * half, half)], d_ref.at[k], d_s.at[k], d_r.at[k], partner)

    def i_copy(k, e):
        return remote(g_ref.at[k, piece(chip_o, e)], i_ref.at[k, e], i_s.at[k, e], i_r.at[k, e], device[e])

    def ii_copy(k, e):
        return remote(g_ref.at[k, piece(toward[e], 1 - e)], q_ref.at[k, e, 1 - e], ii_s.at[k, e], ii_r.at[k, e], device[e])

    def iii_copy(k, e):
        return remote(i_ref.at[k, e], q_ref.at[k, e, e], iii_s.at[k, e], iii_r.at[k, e], device[e])

    def ag1_copy(k, e, c):
        span = go.at[k, pl.ds(piece(c, 0), 2)]
        return remote(span, span, ag1_s.at[k, e], ag1_r.at[k, e], device[e])

    def ag2_copy(k, e, c):
        span = go.at[k, piece(c, e)]
        return remote(span, span, ag2_s.at[k, e], ag2_r.at[k, e], device[e])

    def p_copy(k, j, c, owner):
        span = go.at[k, pl.ds(owner * half + 2 * c, 2)]
        return remote(span, span, p_s.at[k, j], p_r.at[k, j], partner)

    def left_load(k, slot):
        return pltpu.make_async_copy(turned.at[(2 * k + 1) // 3], left_op.at[slot], op_sem.at[slot])

    def right_load(t):
        k, c = t // chunks, lax.rem(t, chunks)
        c = lax.rem(c + (1 - core) * (chunks // 2), chunks)
        return pltpu.make_async_copy(wide.at[k, c], right_op.at[lax.rem(t, 3)], op_sem.at[2 + lax.rem(t, 3)])

    barrier = pltpu.get_barrier_semaphore()
    for to in (*device, partner):
        pl.semaphore_signal(barrier, inc=1, device_id={"dp": to}, device_id_type=MESH)
    left_load(0, 0).start()
    right_load(0).start()
    right_load(1).start()
    pl.semaphore_wait(barrier, 3)

    def multiply(k, c):
        t = k * chunks + c
        right_load(t).wait()

        @pl.when(t + 2 < mats * chunks)
        def _():
            right_load(t + 2).start()

        where = lax.rem(c + (1 - core) * (chunks // 2), chunks) * per
        a = left_op[lax.rem(k, 2)]
        for j in range(0, per, 2):
            b = right_op[lax.rem(t, 3), :, j * lanes : (j + 2) * lanes]
            block = dot(a, b).astype(BF)
            g_ref[k, where + j] = block[:, :lanes]
            g_ref[k, where + j + 1] = block[:, lanes:]

    def reduce_1(k):
        d_copy(k).wait_recv()
        for c in (chip_o, chip_r, chip_l, chip):
            for h in range(2):
                one = g_ref[k, piece(c, h)].astype(F32) + d_ref[k, 2 * c + h].astype(F32)
                g_ref[k, piece(c, h)] = one.astype(BF)
        for e in range(2):
            i_copy(k, e).start()
        for e in range(2):
            ii_copy(k, e).start()

    def reduce_2(k):
        for e in range(2):
            i_copy(k, e).wait_recv()
            one = g_ref[k, piece(toward[e], e)].astype(F32) + i_ref[k, e].astype(F32)
            i_ref[k, e] = one.astype(BF)
            iii_copy(k, e).start()

    def reduce_3(k):
        for e in range(2):
            ii_copy(k, e).wait_recv()
            iii_copy(k, e).wait_recv()

        def total(h):
            one = g_ref[k, piece(chip, h)].astype(F32) + q_ref[k, 0, h].astype(F32) + q_ref[k, 1, h].astype(F32)
            return one.astype(BF)

        @pl.when(k < early)
        def _():
            for h in range(2):
                go[k, piece(chip, h)] = total(h)
            for e in range(2):
                ag1_copy(k, e, chip).start()
            p_copy(k, 0, chip, core).start()

        @pl.when(k >= early)
        def _():
            for h in range(2):
                own[h, k - early] = total(h)
            for h in range(2):
                own_copy(k - early, h).start()

    def own_copy(k, h):
        return pltpu.make_async_copy(own.at[h, k], shards[h].at[k], own_sem.at[k, h])

    def gather_2(k):
        for e in range(2):
            ag1_copy(k, e, behind[e]).wait_recv()
            ag2_copy(k, e, behind[e]).start()
            p_copy(k, 1 + e, behind[e], core).start()

    def gather_3(k):
        for e in range(2):
            ag2_copy(k, e, chip_o).wait_recv()
        p_copy(k, 3, chip_o, core).start()

    def done_copy(k):
        return pltpu.make_async_copy(go.at[k], out.at[k], out_sem.at[k])

    def finish(k):
        for j, c in enumerate((chip, *behind, chip_o)):
            p_copy(k, j, c, 1 - core).wait_recv()
        done_copy(k).start()

    def when(condition):
        return pl.when(condition)

    def step(k, carry):
        @when(k < mats)
        def _():
            left_load(k, lax.rem(k, 2)).wait()

            @when(k + 1 < mats)
            def _():
                left_load(k + 1, lax.rem(k + 1, 2)).start()

            lax.fori_loop(0, chunks // 2, lambda c, _: multiply(k, c), None)
            d_copy(k).start()

        @when(k >= 1)
        def _():
            reduce_2(k - 1)

        @when(k < mats)
        def _():
            lax.fori_loop(chunks // 2, chunks, lambda c, _: multiply(k, c), None)
            reduce_1(k)

        @when(k >= mats + 1 - early)
        def _():
            gather_2(k - (mats + 1 - early))

        @when(k >= 1)
        def _():
            reduce_3(k - 1)

        return carry

    lax.fori_loop(0, mats + 1, step, 0)
    lax.fori_loop(0, early, lambda k, _: gather_3(k), None)
    lax.fori_loop(0, early, lambda k, _: finish(k), None)

    def drain(k, carry):
        d_copy(k).wait_send()
        for e in range(2):
            i_copy(k, e).wait_send()
            ii_copy(k, e).wait_send()
            iii_copy(k, e).wait_send()
        return carry

    def drain_early(k, carry):
        for e in range(2):
            ag1_copy(k, e, chip).wait_send()
            ag2_copy(k, e, behind[e]).wait_send()
        for j, c in enumerate((chip, *behind, chip_o)):
            p_copy(k, j, c, core).wait_send()
        done_copy(k).wait()
        return carry

    def drain_late(k, carry):
        for h in range(2):
            own_copy(k, h).wait()
        return carry

    lax.fori_loop(0, mats, drain, 0)
    lax.fori_loop(0, early, drain_early, 0)
    lax.fori_loop(0, mats - early, drain_late, 0)


def gradients(wide, turned, n):
    mats, chunks, tokens, chunk = wide.shape
    d = turned.shape[1]
    early = late = mats // 2
    pieces = 2 * n
    lanes = chunks * chunk // pieces
    dma = lambda *shape: pltpu.SemaphoreType.DMA(shape)
    pairs = [dma(mats), dma(mats)] + [dma(mats, 2)] * 6 + [dma(early, 2)] * 4 + [dma(early, 4)] * 2
    return pl.pallas_call(
        functools.partial(sum_kernel, n),
        name="gradients",
        in_specs=[pl.BlockSpec(memory_space=pl.ANY)] * 2,
        out_specs=[pl.BlockSpec(memory_space=pl.ANY)] * 3,
        out_shape=[jax.ShapeDtypeStruct((early, pieces, d, lanes), BF)] + [jax.ShapeDtypeStruct((late, d, lanes), BF)] * 2,
        scratch_shapes=[
            pltpu.VMEM((mats, pieces, d, lanes), BF),
            pltpu.VMEM((mats, pieces // 2, d, lanes), BF),
            pltpu.VMEM((mats, 2, d, lanes), BF),
            pltpu.VMEM((mats, 2, 2, d, lanes), BF),
            pltpu.VMEM((early, pieces, d, lanes), BF),
            pltpu.VMEM((2, late, d, lanes), BF),
            pltpu.VMEM((2, d, tokens), BF),
            pltpu.VMEM((3, tokens, chunk), BF),
            dma(5),
            dma(early),
            dma(late, 2),
            *pairs,
        ],
        compiler_params=pltpu.CompilerParams(collective_id=0, has_side_effects=True, vmem_limit_bytes=VMEM_LIMIT),
    )(wide, turned)


def adamw(w, m, v, g):
    m = 0.9 * m + 0.1 * g
    v = 0.95 * v + 0.05 * g * g
    step = m * lax.rsqrt(v + 1e-8) + 0.1 * w
    return (w - 0.02 * step).astype(BF), m, v


def update_kernel(n, layer, jobs, given, slots, *refs):
    sources, ins, outs = refs[:given], refs[given : given + 9], refs[-19:-10]
    bufs, in_sem, out_sem = refs[-10:-2], refs[-2], refs[-1]
    me = lax.axis_index("dp")
    chips = n // 2
    lanes = sources[0].shape[-1]
    width = 2 * lanes

    def shards(job):
        a, s, where = job
        mat = (a + 1) % 3
        if where is None:
            return [sources[0].at[mat, 2 * s + h] for h in range(2)]
        return [sources[2 * s + h].at[mat] for h in range(2)]

    def spot(i):
        a, s, where = jobs[i]
        tall = a == 2
        slot = len([1 for job in jobs[:i] if (job[0] == 2) == tall]) % slots
        if where is None:
            block = s
        else:
            block = lax.rem(lax.rem(me, 2) + where[0], 2) * chips + lax.rem(me // 2 + where[1], chips)
        span = pl.ds(pl.multiple_of(block * width, width), width)
        at = (layer, span) if tall else (layer, slice(None), span)
        return at, slot + slots * tall, [b.at[slot] for b in bufs[4 * tall : 4 * tall + 4]]

    def loads(i):
        a = jobs[i][0]
        at, slot, (g, *held) = spot(i)
        pairs = [(ins[a + 3 * k].at[at], held[k]) for k in range(3)] + [(x, g.at[h]) for h, x in enumerate(shards(jobs[i]))]
        return [pltpu.make_async_copy(x, y, in_sem.at[5 * slot + k]) for k, (x, y) in enumerate(pairs)]

    def stores(i):
        a = jobs[i][0]
        at, slot, (_, *held) = spot(i)
        return [pltpu.make_async_copy(held[k], outs[a + 3 * k].at[at], out_sem.at[3 * slot + k]) for k in range(3)]

    def before(i):
        tall = jobs[i][0] == 2
        same = [k for k in range(i) if (jobs[k][0] == 2) == tall]
        return same[-slots] if len(same) >= slots else None

    def start(i):
        k = before(i)
        if k is not None:
            for c in stores(k):
                c.wait()
        for c in loads(i):
            c.start()

    ahead = slots // 2 + 1
    for i in range(min(ahead, len(jobs))):
        start(i)
    for i, (a, _, _) in enumerate(jobs):
        if i + ahead < len(jobs):
            start(i + ahead)
        g, w, m, v = spot(i)[2]
        for c in loads(i):
            c.wait()
        if a == 2:
            count = w.shape[1] // lanes

            def rows(t, _):
                h, q = t // count, lax.rem(t, count)
                cols = pl.ds(pl.multiple_of(q * lanes, lanes), lanes)
                at = (pl.ds(pl.multiple_of(h * lanes, lanes), lanes), cols)
                w[at], m[at], v[at] = adamw(w[at].astype(F32), m[at], v[at], g[h, cols].astype(F32).T)

            lax.fori_loop(0, 2 * count, rows, None)
        else:
            high = 64

            def rows(t, _):
                span = pl.ds(pl.multiple_of(t * high, high), high)
                for h in range(2):
                    at = (span, pl.ds(h * lanes, lanes))
                    w[at], m[at], v[at] = adamw(w[at].astype(F32), m[at], v[at], g[h, span].astype(F32))

            lax.fori_loop(0, w.shape[0] // high, rows, None)
        for c in stores(i):
            c.start()
    for i in range(len(jobs)):
        if all(before(k) != i for k in range(len(jobs))):
            for c in stores(i):
                c.wait()


def update(n, sources, places, layer, arrays, new=()):
    _, d, ff = arrays[0].shape
    width = ff // n
    if places is None:
        jobs = [(a, s, None) for s in range(n) for a in (2, 0, 1)]
    else:
        jobs = [(a, s, place) for s, place in enumerate(places) for a in (2, 0, 1)]
        sources = [x for pair in sources for x in pair]
    depth = 8
    kinds = (BF, BF, F32, F32)
    held = [pltpu.VMEM((depth, *shape), kind) for low in ((d, width), (width, d)) for kind, shape in zip(kinds, ((2, d, width // 2), low, low, low))]
    given = len(sources)
    elements = len(jobs) * d * width
    return pl.pallas_call(
        functools.partial(update_kernel, n, layer, jobs, given, depth),
        name="update",
        in_specs=[pl.BlockSpec(memory_space=pl.ANY)] * (given + 9 + len(new)),
        out_specs=[pl.BlockSpec(memory_space=pl.ANY)] * 9,
        out_shape=[jax.ShapeDtypeStruct(x.shape, x.dtype) for x in arrays],
        input_output_aliases={given + 9 + i: i for i in range(len(new))},
        scratch_shapes=[*held, pltpu.SemaphoreType.DMA((10 * depth,)), pltpu.SemaphoreType.DMA((6 * depth,))],
        cost_estimate=pl.CostEstimate(flops=150 * elements, bytes_accessed=22 * elements, transcendentals=elements),
        compiler_params=pltpu.CompilerParams(vmem_limit_bytes=VMEM_LIMIT),
    )(*sources, *arrays, *new)


def solution(mesh):
    n = mesh.shape["dp"]
    chips = n // 2
    to_right = [(i, (i + 2) % n) for i in range(n)]
    to_left = [(i, (i - 2) % n) for i in range(n)]
    across = [(i, i ^ 1) for i in range(n)]

    def send(pair, to):
        return tuple(lax.ppermute(x, "dp", to) for x in pair)

    def step(x, dy, *arrays):
        weights = arrays[:3]
        wide, turned = chain(x[0], dy[0], *weights)
        g, *own = gradients(wide, turned, n)
        left, right, other = send(own, to_right), send(own, to_left), send(own, across)
        new = update(n, [g], None, 1, arrays)
        left, right, first = lax.optimization_barrier((left, right, new[0]))
        new = [first, *new[1:]]
        far = (*send(left[:1], to_right), *send(right[1:], to_left))
        other_left, other_right = send(left, across), send(right, across)
        new = update(n, [own, other, left, right], [(0, 0), (1, 0), (0, chips - 1), (0, 1)], 0, arrays, new)
        far, first = lax.optimization_barrier((far, new[0]))
        new = [first, *new[1:]]
        other_far = send(far, across)
        new = update(n, [other_left, other_right, far], [(1, chips - 1), (1, 1), (0, 2)], 0, arrays, new)
        return tuple(update(n, [other_far], [(1, 2)], 0, arrays, new))

    return jax.shard_map(
        step,
        mesh=mesh,
        in_specs=(P(("rep", "dp"), None, None),) * 2 + (P(None, None, None),) * 9,
        out_specs=(P("rep", None, None),) * 9,
        check_vma=False,
    )
```

```python
import functools

import jax
import jax.numpy as jnp
from jax import lax
from jax.experimental import pallas as pl
from jax.experimental.pallas import tpu as pltpu
from jax.sharding import PartitionSpec as P

BF, F32 = jnp.bfloat16, jnp.float32
MESH = pl.DeviceIdType.MESH
VMEM_LIMIT = 64 * 1024 * 1024 - 256 * 1024


def dot(a, b):
    return lax.dot_general(a, b, (((1,), (0,)), ((), ())), preferred_element_type=F32)


def dot_t(a, b):
    return lax.dot_general(a, b, (((1,), (1,)), ((), ())), preferred_element_type=F32)


def norm(h):
    wide = h.astype(F32)
    scale = lax.rsqrt(jnp.mean(wide * wide, -1, keepdims=True) + 1e-6)
    return (wide * scale).astype(BF)


def chain_kernel(chunk, x_ref, dy_ref, wg, wu, wd, wide, turned, silu_1, slope_1):
    p2, dg2, du2, p1 = (wide.at[i] for i in range(4))
    dyt, a2t, h1t, a1t = (turned.at[i] for i in range(4))
    chunks = wg.shape[-1] // chunk
    shape = wide.shape[2:]
    x = x_ref[...]
    a1 = norm(x)
    a1t[...] = a1.T
    down = None
    for c in range(chunks):
        cols = pl.ds(c * chunk, chunk)
        g = dot(a1, wg[0, :, cols])
        u = dot(a1, wu[0, :, cols])
        s = jax.nn.sigmoid(g)
        silu = g * s
        p = (silu * u).astype(BF)
        p1[c] = p.reshape(shape)
        silu_1[c] = silu.reshape(shape)
        slope_1[c] = (u * (s * (1.0 + g * (1.0 - s)))).reshape(shape)
        term = dot(p, wd[0, cols, :])
        down = term if down is None else down + term
    h1 = x + down.astype(BF)
    h1t[...] = h1.T
    a2 = norm(h1)
    a2t[...] = a2.T
    dy = dy_ref[...]
    dyt[...] = dy.T
    for c in range(chunks):
        cols = pl.ds(c * chunk, chunk)
        g = dot(a2, wg[1, :, cols])
        u = dot(a2, wu[1, :, cols])
        dp = dot_t(dy, wd[1, cols, :]).astype(BF).astype(F32)
        s = jax.nn.sigmoid(g)
        silu = g * s
        p2[c] = (silu * u).astype(BF).reshape(shape)
        du2[c] = (dp * silu).astype(BF).reshape(shape)
        dg2[c] = (dp * (u * (s * (1.0 + g * (1.0 - s))))).astype(BF).reshape(shape)


def chain(x, dy, wg, wu, wd, tile=512, chunk=512, step=256):
    tokens, d = x.shape
    chunks = wg.shape[-1] // chunk
    whole = lambda w: pl.BlockSpec(w.shape, lambda i: (0, 0, 0), pipeline_mode=pl.Buffered(1))
    rows = pl.BlockSpec((tile, d), lambda i: (i, 0))
    factor = pl.BlockSpec((chunks, tile // step, step, chunk), lambda i: (0, i, 0, 0))
    return pl.pallas_call(
        functools.partial(chain_kernel, chunk),
        name="chain",
        grid=(tokens // tile,),
        in_specs=[rows, rows, whole(wg), whole(wu), whole(wd)],
        out_specs=[
            pl.BlockSpec((4, chunks, tile // step, step, chunk), lambda i: (0, 0, i, 0, 0)),
            pl.BlockSpec((4, d, tile), lambda i: (0, 0, i)),
            factor,
            factor,
        ],
        out_shape=[
            jax.ShapeDtypeStruct((4, chunks, tokens // step, step, chunk), BF),
            jax.ShapeDtypeStruct((4, d, tokens), BF),
            jax.ShapeDtypeStruct((chunks, tokens // step, step, chunk), F32),
            jax.ShapeDtypeStruct((chunks, tokens // step, step, chunk), F32),
        ],
        compiler_params=pltpu.CompilerParams(dimension_semantics=("arbitrary",), vmem_limit_bytes=VMEM_LIMIT),
    )(x, dy, wg, wu, wd)


def sum_kernel(n, wide, turned, silu_1, slope_1, wg, wu, wd, out, shard_a, shard_b, wide_1, *refs):
    g_ref, d_ref, i_ref, q_ref, go, own, left_op, right_op, wg_1, wu_1, wd_0, factors, thin, *sems = refs
    (op_sem, w_sem, tile_sem, stage_sem, out_sem, own_sem, d_s, d_r, i_s, i_r, ii_s, ii_r, iii_s, iii_r, ag1_s, ag1_r, ag2_s, ag2_r, p_s, p_r) = sems
    _, chunks, tiles, rows, chunk = wide.shape
    tokens, d = tiles * rows, turned.shape[1]
    mats, first = g_ref.shape[0], g_ref.shape[0] // 2
    early = go.shape[0]
    shards = (shard_a, shard_b)
    pieces = g_ref.shape[1]
    half = pieces // 2
    per = pieces // chunks
    lanes = g_ref.shape[-1]
    me = lax.axis_index("dp")
    core = lax.rem(me, 2)
    chip = me // 2
    chips = n // 2
    partner = me + 1 - 2 * core
    chip_r = lax.rem(chip + 1, chips)
    chip_l = lax.rem(chip + chips - 1, chips)
    chip_o = lax.rem(chip + 2, chips)
    toward = (chip_r, chip_l)
    behind = (chip_l, chip_r)
    device = tuple(2 * c + core for c in toward)

    def piece(c, h):
        return core * half + 2 * c + h

    def remote(src, dst, s, r, to):
        return pltpu.make_async_remote_copy(src, dst, s, r, device_id={"dp": to}, device_id_type=MESH)

    def d_copy(k):
        return remote(g_ref.at[k, pl.ds((1 - core) * half, half)], d_ref.at[k], d_s.at[k], d_r.at[k], partner)

    def i_copy(k, e):
        return remote(g_ref.at[k, piece(chip_o, e)], i_ref.at[k, e], i_s.at[k, e], i_r.at[k, e], device[e])

    def ii_copy(k, e):
        return remote(g_ref.at[k, piece(toward[e], 1 - e)], q_ref.at[k, e, 1 - e], ii_s.at[k, e], ii_r.at[k, e], device[e])

    def iii_copy(k, e):
        return remote(i_ref.at[k, e], q_ref.at[k, e, e], iii_s.at[k, e], iii_r.at[k, e], device[e])

    def ag1_copy(k, e, c):
        span = go.at[k, pl.ds(piece(c, 0), 2)]
        return remote(span, span, ag1_s.at[k, e], ag1_r.at[k, e], device[e])

    def ag2_copy(k, e, c):
        span = go.at[k, piece(c, e)]
        return remote(span, span, ag2_s.at[k, e], ag2_r.at[k, e], device[e])

    def p_copy(k, j, c, owner):
        span = go.at[k, pl.ds(owner * half + 2 * c, 2)]
        return remote(span, span, p_s.at[k, j], p_r.at[k, j], partner)

    def left_load(k, slot):
        return pltpu.make_async_copy(turned.at[(2 * k + 1) // 3], left_op.at[slot], op_sem.at[slot])

    def right_copy(t, later):
        k, c = t // chunks, lax.rem(t, chunks)
        c = lax.rem(c + (1 - core) * (chunks // 2), chunks)
        slot = lax.rem(t, 3)
        return pltpu.make_async_copy(wide_1.at[k - first - 1, c] if later else wide.at[k, c], right_op.at[slot], op_sem.at[2 + slot])

    def right_load(t):
        @pl.when(t < (first + 1) * chunks)
        def _():
            right_copy(t, False).start()

        @pl.when(t >= (first + 1) * chunks)
        def _():
            right_copy(t, True).start()

    weights = [
        pltpu.make_async_copy(wg.at[1], wg_1, w_sem.at[0]),
        pltpu.make_async_copy(wu.at[1], wu_1, w_sem.at[1]),
        pltpu.make_async_copy(wd.at[0], wd_0, w_sem.at[2]),
    ]

    def tile_loads(i):
        odd = lax.rem(i, 2)
        span = pl.ds(pl.multiple_of(i * rows, rows), rows)
        half_slot = pl.ds(odd * chunks, chunks)
        pairs = [
            (wide.at[1, :, i], right_op.at[0, half_slot]),
            (wide.at[2, :, i], right_op.at[1, half_slot]),
            (silu_1.at[:, i], factors.at[0, odd]),
            (slope_1.at[:, i], factors.at[1, odd]),
            (turned.at[0, :, span], thin.at[0, odd]),
            (turned.at[2, :, span], thin.at[1, odd]),
        ]
        return [pltpu.make_async_copy(x, y, tile_sem.at[odd, j]) for j, (x, y) in enumerate(pairs)]

    def stages(i):
        return [pltpu.make_async_copy(right_op.at[2, pl.ds(j * chunks, chunks)], wide_1.at[j, :, i], stage_sem.at[j]) for j in range(2)]

    barrier = pltpu.get_barrier_semaphore()
    for to in (*device, partner):
        pl.semaphore_signal(barrier, inc=1, device_id={"dp": to}, device_id_type=MESH)
    left_load(0, 0).start()
    right_load(0)
    right_load(1)
    for c in weights:
        c.start()
    pl.semaphore_wait(barrier, 3)

    def multiply(t):
        k, c = t // chunks, lax.rem(t, chunks)

        @pl.when((c == 0) & (k != first))
        def _():
            left_load(k, lax.rem(k, 2)).wait()

        @pl.when((c == 0) & (k + 1 != first) & (k + 1 < mats))
        def _():
            left_load(k + 1, lax.rem(k + 1, 2)).start()

        pltpu.make_async_copy(wide.at[0, 0], right_op.at[lax.rem(t, 3)], op_sem.at[2 + lax.rem(t, 3)]).wait()

        @pl.when((t + 2 < first * chunks) | ((t >= first * chunks) & (t + 2 < mats * chunks)))
        def _():
            right_load(t + 2)

        where = lax.rem(c + (1 - core) * (chunks // 2), chunks) * per
        a = left_op[lax.rem(k, 2)]
        for j in range(0, per, 2):
            b = right_op[lax.rem(t, 3), :, :, j * lanes : (j + 2) * lanes].reshape(tokens, 2 * lanes)
            block = dot(a, b).astype(BF)
            g_ref[k, where + j] = block[:, :lanes]
            g_ref[k, where + j + 1] = block[:, lanes:]

        @pl.when(c == chunks // 2 - 1)
        def _():
            d_copy(k).start()

    def tile_of_layer_0(i):
        odd = lax.rem(i, 2)
        for c in tile_loads(i):
            c.wait()

        @pl.when(i + 1 < tiles)
        def _():
            for c in tile_loads(i + 1):
                c.start()

        dag = dau = None
        for c in range(chunks):
            cols = pl.ds(c * chunk, chunk)
            tg = dot_t(wg_1[:, cols], right_op[0, odd * chunks + c])
            tu = dot_t(wu_1[:, cols], right_op[1, odd * chunks + c])
            dag = tg if dag is None else dag + tg
            dau = tu if dau is None else dau + tu

        @pl.when(i + 1 == tiles)
        def _():
            right_load(first * chunks)
            right_load(first * chunks + 1)

        da = (dag.astype(BF) + dau.astype(BF)).astype(F32)
        high = thin[1, odd].astype(F32)
        scale = lax.rsqrt(jnp.mean(high * high, 0, keepdims=True) + 1e-6)
        slope = jnp.sum(da * high, 0, keepdims=True)
        change = da * scale - high * (scale * scale * scale * slope * (1.0 / d))
        dh = thin[0, odd] + change.astype(BF)
        left_op[first % 2, :, pl.ds(pl.multiple_of(i * rows, rows), rows)] = dh
        dh = dh.T

        @pl.when(i > 0)
        def _():
            for c in stages(i - 1):
                c.wait()

        for c in range(chunks):
            dp = dot_t(dh, wd_0[c * chunk : (c + 1) * chunk]).astype(BF).astype(F32)
            right_op[2, c] = (dp * factors[1, odd, c]).astype(BF)
            right_op[2, chunks + c] = (dp * factors[0, odd, c]).astype(BF)
        for c in stages(i):
            c.start()

    def reduce_1(k):
        d_copy(k).wait_recv()
        for c in (chip_o, chip_r, chip_l, chip):
            for h in range(2):
                one = g_ref[k, piece(c, h)].astype(F32) + d_ref[k, 2 * c + h].astype(F32)
                g_ref[k, piece(c, h)] = one.astype(BF)
        for e in range(2):
            i_copy(k, e).start()
        for e in range(2):
            ii_copy(k, e).start()

    def reduce_2(k):
        for e in range(2):
            i_copy(k, e).wait_recv()
            one = g_ref[k, piece(toward[e], e)].astype(F32) + i_ref[k, e].astype(F32)
            i_ref[k, e] = one.astype(BF)
            iii_copy(k, e).start()

    def reduce_3(k):
        for e in range(2):
            ii_copy(k, e).wait_recv()
            iii_copy(k, e).wait_recv()

        def total(h):
            one = g_ref[k, piece(chip, h)].astype(F32) + q_ref[k, 0, h].astype(F32) + q_ref[k, 1, h].astype(F32)
            return one.astype(BF)

        @pl.when(k < early)
        def _():
            for h in range(2):
                go[k, piece(chip, h)] = total(h)
            for e in range(2):
                ag1_copy(k, e, chip).start()
            p_copy(k, 0, chip, core).start()

        @pl.when(k >= early)
        def _():
            for h in range(2):
                own[h, k - early] = total(h)
            for h in range(2):
                own_copy(k - early, h).start()

    def own_copy(k, h):
        return pltpu.make_async_copy(own.at[h, k], shards[h].at[k], own_sem.at[k, h])

    def gather_2(k):
        for e in range(2):
            ag1_copy(k, e, behind[e]).wait_recv()
            ag2_copy(k, e, behind[e]).start()
            p_copy(k, 1 + e, behind[e], core).start()

    def gather_3(k):
        for e in range(2):
            ag2_copy(k, e, chip_o).wait_recv()
        p_copy(k, 3, chip_o, core).start()

    def done_copy(k):
        return pltpu.make_async_copy(go.at[k], out.at[k], out_sem.at[k])

    def finish(k):
        for j, c in enumerate((chip, *behind, chip_o)):
            p_copy(k, j, c, 1 - core).wait_recv()
        done_copy(k).start()

    def last_chunk(t):
        return lax.rem(t, chunks) == chunks - 1

    def first_half(t, carry):
        multiply(t)
        k = t // chunks

        @pl.when(last_chunk(t))
        def _():
            reduce_1(k)

            @pl.when(k > 0)
            def _():
                reduce_2(k - 1)

        return carry

    def middle(i, carry):
        tile_of_layer_0(i)

        @pl.when(i == 1)
        def _():
            reduce_2(first - 1)
            reduce_3(0)

        @pl.when(i == 4)
        def _():
            reduce_3(1)

        @pl.when(i == 5)
        def _():
            reduce_3(2)

        @pl.when(i == 6)
        def _():
            gather_2(0)

        return carry

    def second_half(t, carry):
        multiply(t)
        k = t // chunks

        @pl.when(last_chunk(t))
        def _():
            reduce_1(k)

            @pl.when(k == first)
            def _():
                gather_2(1)

            @pl.when(k > first)
            def _():
                reduce_2(k - 1)

        return carry

    lax.fori_loop(0, first * chunks, first_half, 0)
    for c in weights:
        c.wait()
    for c in tile_loads(0):
        c.start()
    lax.fori_loop(0, tiles, middle, 0)
    for c in stages(tiles - 1):
        c.wait()
    lax.fori_loop(first * chunks, mats * chunks, second_half, 0)
    reduce_2(mats - 1)
    lax.fori_loop(first, mats - 1, lambda k, _: reduce_3(k), None)
    lax.fori_loop(0, early, lambda k, _: gather_3(k), None)
    lax.fori_loop(0, early, lambda k, _: finish(k), None)
    reduce_3(mats - 1)

    def drain(k, carry):
        d_copy(k).wait_send()
        for e in range(2):
            i_copy(k, e).wait_send()
            ii_copy(k, e).wait_send()
            iii_copy(k, e).wait_send()
        return carry

    def drain_early(k, carry):
        for e in range(2):
            ag1_copy(k, e, chip).wait_send()
            ag2_copy(k, e, behind[e]).wait_send()
        for j, c in enumerate((chip, *behind, chip_o)):
            p_copy(k, j, c, core).wait_send()
        done_copy(k).wait()
        return carry

    def drain_late(k, carry):
        for h in range(2):
            own_copy(k, h).wait()
        return carry

    lax.fori_loop(0, mats, drain, 0)
    lax.fori_loop(0, early, drain_early, 0)
    lax.fori_loop(0, mats - early, drain_late, 0)


def gradients(wide, turned, silu_1, slope_1, weights, n, early=2):
    _, chunks, tiles, rows, chunk = wide.shape
    d, tokens = turned.shape[1:]
    mats = 6
    late = mats - early
    pieces = 2 * n
    lanes = chunks * chunk // pieces
    dma = lambda *shape: pltpu.SemaphoreType.DMA(shape)
    return pl.pallas_call(
        functools.partial(sum_kernel, n),
        name="gradients",
        in_specs=[pl.BlockSpec(memory_space=pl.ANY)] * 7,
        out_specs=[pl.BlockSpec(memory_space=pl.ANY)] * 4,
        out_shape=[
            jax.ShapeDtypeStruct((early, pieces, d, lanes), BF),
            jax.ShapeDtypeStruct((late, d, lanes), BF),
            jax.ShapeDtypeStruct((late, d, lanes), BF),
            jax.ShapeDtypeStruct((2, chunks, tiles, rows, chunk), BF),
        ],
        scratch_shapes=[
            pltpu.VMEM((mats, pieces, d, lanes), BF),
            pltpu.VMEM((mats, pieces // 2, d, lanes), BF),
            pltpu.VMEM((mats, 2, d, lanes), BF),
            pltpu.VMEM((mats, 2, 2, d, lanes), BF),
            pltpu.VMEM((early, pieces, d, lanes), BF),
            pltpu.VMEM((2, late, d, lanes), BF),
            pltpu.VMEM((2, d, tokens), BF),
            pltpu.VMEM((3, tiles, rows, chunk), BF),
            pltpu.VMEM(weights[0].shape[1:], BF),
            pltpu.VMEM(weights[1].shape[1:], BF),
            pltpu.VMEM(weights[2].shape[1:], BF),
            pltpu.VMEM((2, 2, chunks, rows, chunk), F32),
            pltpu.VMEM((2, 2, d, rows), BF),
            dma(5),
            dma(3),
            dma(2, 6),
            dma(2),
            dma(early),
            dma(late, 2),
            dma(mats),
            dma(mats),
            *[dma(mats, 2)] * 6,
            *[dma(early, 2)] * 4,
            *[dma(early, 4)] * 2,
        ],
        compiler_params=pltpu.CompilerParams(collective_id=0, has_side_effects=True, vmem_limit_bytes=VMEM_LIMIT),
    )(wide, turned, silu_1, slope_1, *weights)[:3]


def adamw(w, m, v, g):
    m = 0.9 * m + 0.1 * g
    v = 0.95 * v + 0.05 * g * g
    step = m * lax.rsqrt(v + 1e-8) + 0.1 * w
    return (w - 0.02 * step).astype(BF), m, v


def update_kernel(n, jobs, given, slots, *refs):
    sources, ins, outs = refs[:given], refs[given : given + 9], refs[-19:-10]
    bufs, in_sem, out_sem = refs[-10:-2], refs[-2], refs[-1]
    me = lax.axis_index("dp")
    chips = n // 2
    lanes = sources[0].shape[-1]
    width = 2 * lanes

    def shards(job):
        _, _, mat, s, where = job
        if isinstance(where, int):
            return [sources[s].at[mat, 2 * where + h] for h in range(2)]
        return [sources[s + h].at[mat] for h in range(2)]

    def spot(i):
        a, layer, _, _, where = jobs[i]
        tall = a == 2
        slot = len([1 for job in jobs[:i] if (job[0] == 2) == tall]) % slots
        if isinstance(where, int):
            block = where
        else:
            block = lax.rem(lax.rem(me, 2) + where[0], 2) * chips + lax.rem(me // 2 + where[1], chips)
        span = pl.ds(pl.multiple_of(block * width, width), width)
        at = (layer, span) if tall else (layer, slice(None), span)
        return at, slot + slots * tall, [b.at[slot] for b in bufs[4 * tall : 4 * tall + 4]]

    def loads(i):
        a = jobs[i][0]
        at, slot, (g, *held) = spot(i)
        pairs = [(ins[a + 3 * k].at[at], held[k]) for k in range(3)] + [(x, g.at[h]) for h, x in enumerate(shards(jobs[i]))]
        return [pltpu.make_async_copy(x, y, in_sem.at[5 * slot + k]) for k, (x, y) in enumerate(pairs)]

    def stores(i):
        a = jobs[i][0]
        at, slot, (_, *held) = spot(i)
        return [pltpu.make_async_copy(held[k], outs[a + 3 * k].at[at], out_sem.at[3 * slot + k]) for k in range(3)]

    def before(i):
        tall = jobs[i][0] == 2
        same = [k for k in range(i) if (jobs[k][0] == 2) == tall]
        return same[-slots] if len(same) >= slots else None

    def start(i):
        k = before(i)
        if k is not None:
            for c in stores(k):
                c.wait()
        for c in loads(i):
            c.start()

    ahead = slots // 2 + 1
    for i in range(min(ahead, len(jobs))):
        start(i)
    for i, (a, *_) in enumerate(jobs):
        if i + ahead < len(jobs):
            start(i + ahead)
        g, w, m, v = spot(i)[2]
        for c in loads(i):
            c.wait()
        if a == 2:
            count = w.shape[1] // lanes

            def rows(t, _):
                h, q = t // count, lax.rem(t, count)
                cols = pl.ds(pl.multiple_of(q * lanes, lanes), lanes)
                at = (pl.ds(pl.multiple_of(h * lanes, lanes), lanes), cols)
                w[at], m[at], v[at] = adamw(w[at].astype(F32), m[at], v[at], g[h, cols].astype(F32).T)

            lax.fori_loop(0, 2 * count, rows, None)
        else:
            high = 64

            def rows(t, _):
                span = pl.ds(pl.multiple_of(t * high, high), high)
                for h in range(2):
                    at = (span, pl.ds(h * lanes, lanes))
                    w[at], m[at], v[at] = adamw(w[at].astype(F32), m[at], v[at], g[h, span].astype(F32))

            lax.fori_loop(0, w.shape[0] // high, rows, None)
        for c in stores(i):
            c.start()
    for i in range(len(jobs)):
        if all(before(k) != i for k in range(len(jobs))):
            for c in stores(i):
                c.wait()


def update(n, whole, pairs, places, kinds_of, arrays, new=()):
    _, d, ff = arrays[0].shape
    width = ff // n
    sources = [*whole, *[x for pair in pairs for x in pair]]
    count = len(kinds_of) - pairs[0][0].shape[0]
    jobs = [(*kinds_of[k], k, 0, s) for s in range(n) for k in range(count)] if whole else []
    jobs += [(*kinds, k, len(whole) + 2 * s, place) for s, place in enumerate(places) for k, kinds in enumerate(kinds_of[count:])]
    depth = 8
    kinds = (BF, BF, F32, F32)
    held = [pltpu.VMEM((depth, *shape), kind) for low in ((d, width), (width, d)) for kind, shape in zip(kinds, ((2, d, width // 2), low, low, low))]
    given = len(sources)
    elements = len(jobs) * d * width
    return pl.pallas_call(
        functools.partial(update_kernel, n, jobs, given, depth),
        name="update",
        in_specs=[pl.BlockSpec(memory_space=pl.ANY)] * (given + 9 + len(new)),
        out_specs=[pl.BlockSpec(memory_space=pl.ANY)] * 9,
        out_shape=[jax.ShapeDtypeStruct(x.shape, x.dtype) for x in arrays],
        input_output_aliases={given + 9 + i: i for i in range(len(new))},
        scratch_shapes=[*held, pltpu.SemaphoreType.DMA((10 * depth,)), pltpu.SemaphoreType.DMA((6 * depth,))],
        cost_estimate=pl.CostEstimate(flops=150 * elements, bytes_accessed=22 * elements, transcendentals=elements),
        compiler_params=pltpu.CompilerParams(vmem_limit_bytes=VMEM_LIMIT),
    )(*sources, *arrays, *new)


def solution(mesh):
    n = mesh.shape["dp"]
    chips = n // 2
    to_right = [(i, (i + 2) % n) for i in range(n)]
    to_left = [(i, (i - 2) % n) for i in range(n)]
    across = [(i, i ^ 1) for i in range(n)]
    kinds_of = [(a, layer) for layer in (1, 0) for a in (2, 0, 1)]

    def send(pair, to):
        return tuple(lax.ppermute(x, "dp", to) for x in pair)

    def step(x, dy, *arrays):
        weights = arrays[:3]
        operands = chain(x[0], dy[0], *weights)
        g, *own = gradients(*operands, weights, n)
        left, right, other = send(own, to_right), send(own, to_left), send(own, across)
        new = update(n, [g], [own, other], [(0, 0), (1, 0)], kinds_of, arrays)
        left, right, first = lax.optimization_barrier((left, right, new[0]))
        new = [first, *new[1:]]
        far = (*send(left[:1], to_right), *send(right[1:], to_left))
        other_left, other_right = send(left, across), send(right, across)
        new = update(n, [], [left, right], [(0, chips - 1), (0, 1)], kinds_of, arrays, new)
        far, first = lax.optimization_barrier((far, new[0]))
        new = [first, *new[1:]]
        other_far = send(far, across)
        new = update(n, [], [other_left, other_right, far], [(1, chips - 1), (1, 1), (0, 2)], kinds_of, arrays, new)
        return tuple(update(n, [], [other_far], [(1, 2)], kinds_of, arrays, new))

    return jax.shard_map(
        step,
        mesh=mesh,
        in_specs=(P(("rep", "dp"), None, None),) * 2 + (P(None, None, None),) * 9,
        out_specs=(P("rep", None, None),) * 9,
        check_vma=False,
    )
```

```python
import functools

import jax
import jax.numpy as jnp
from jax import lax
from jax.experimental import pallas as pl
from jax.experimental.pallas import tpu as pltpu
from jax.sharding import PartitionSpec as P

BF, F32 = jnp.bfloat16, jnp.float32
MESH = pl.DeviceIdType.MESH
VMEM_LIMIT = 64 * 1024 * 1024 - 256 * 1024


def dot(a, b):
    return lax.dot_general(a, b, (((1,), (0,)), ((), ())), preferred_element_type=F32)


def dot_t(a, b):
    return lax.dot_general(a, b, (((1,), (1,)), ((), ())), preferred_element_type=F32)


def norm(h):
    wide = h.astype(F32)
    scale = lax.rsqrt(jnp.mean(wide * wide, -1, keepdims=True) + 1e-6)
    return (wide * scale).astype(BF)


def chain_kernel(chunk, x_ref, dy_ref, wg_in, wu_in, wd_in, turned, wdt, wide, silu_1, slope_1, wg, wu, wd, held, factors, w_sem, o_sem, f_sem):
    i = pl.program_id(0)
    steps = pl.num_programs(0)
    dyt, a2t, h1t, a1t = (turned.at[j] for j in range(4))
    chunks = wg.shape[-1] // chunk
    shape = held.shape[2:]
    rows = shape[0]

    def weights(layer):
        return [pltpu.make_async_copy(x.at[layer], y.at[layer], w_sem.at[layer, j]) for j, (x, y) in enumerate(((wg_in, wg), (wu_in, wu), (wd_in, wd)))]

    def early_out(i):
        span = pl.ds(i * rows, rows)
        pairs = ((held.at[3], wide.at[3, :, span]), (factors.at[0], silu_1.at[:, span]), (factors.at[1], slope_1.at[:, span]))
        return [pltpu.make_async_copy(x, y, f_sem.at[j]) for j, (x, y) in enumerate(pairs)]

    def late_out(i, c):
        return [pltpu.make_async_copy(held.at[j, c], wide.at[j, c, pl.ds(i * rows, rows)], o_sem.at[c, j]) for j in range(3)]

    @pl.when(i == 0)
    def _():
        for layer in range(2):
            for w in weights(layer):
                w.start()
        for w in weights(0):
            w.wait()

    @pl.when(i > 0)
    def _():
        for out in early_out(i - 1):
            out.wait()

    x = x_ref[...]
    a1 = norm(x)
    a1t[...] = a1.T
    down = None
    group = 2
    parts = [(j, slice(j * chunk, (j + 1) * chunk)) for j in range(group)]
    for c in range(0, chunks, group):
        cols = pl.ds(c * chunk, group * chunk)
        g = dot(a1, wg[0, :, cols])
        u = dot(a1, wu[0, :, cols])
        s = jax.nn.sigmoid(g)
        silu = g * s
        p = (silu * u).astype(BF)
        slope = u * (s * (1.0 + g * (1.0 - s)))
        for j, part in parts:
            held[3, c + j] = p[:, part].reshape(shape)
            factors[0, c + j] = silu[:, part].reshape(shape)
            factors[1, c + j] = slope[:, part].reshape(shape)
        term = dot(p, wd[0, cols, :])
        down = term if down is None else down + term
    h1 = x + down.astype(BF)
    h1t[...] = h1.T
    a2 = norm(h1)
    a2t[...] = a2.T
    dy = dy_ref[...]
    dyt[...] = dy.T
    turn = wdt.shape[-1]
    wdt[...] = wd[0, pl.ds(pl.multiple_of(i * turn, turn), turn), :].T
    for out in early_out(i):
        out.start()

    @pl.when(i == 0)
    def _():
        for w in weights(1):
            w.wait()

    @pl.when(i > 0)
    def _():
        for c in range(chunks):
            for out in late_out(i - 1, c):
                out.wait()

    for c in range(0, chunks, group):
        cols = pl.ds(c * chunk, group * chunk)
        g = dot(a2, wg[1, :, cols])
        u = dot(a2, wu[1, :, cols])
        dp = dot_t(dy, wd[1, cols, :]).astype(BF).astype(F32)
        s = jax.nn.sigmoid(g)
        silu = g * s
        p = (silu * u).astype(BF)
        du = (dp * silu).astype(BF)
        dg = (dp * (u * (s * (1.0 + g * (1.0 - s))))).astype(BF)
        for j, part in parts:
            held[0, c + j] = p[:, part].reshape(shape)
            held[2, c + j] = du[:, part].reshape(shape)
            held[1, c + j] = dg[:, part].reshape(shape)
        for j in range(group):
            for out in late_out(i, c + j):
                out.start()

    @pl.when(i == steps - 1)
    def _():
        for out in early_out(i):
            out.wait()
        for c in range(chunks):
            for out in late_out(i, c):
                out.wait()


def chain(x, dy, wg, wu, wd, tile=512, chunk=512, step=256):
    tokens, d = x.shape
    ff = wg.shape[-1]
    chunks, count, high = ff // chunk, tokens // tile, tile // step
    anywhere = pl.BlockSpec(memory_space=pl.ANY)
    rows = pl.BlockSpec((tile, d), lambda i: (i, 0))
    turned, wdt, *outs = pl.pallas_call(
        functools.partial(chain_kernel, chunk),
        name="chain",
        grid=(count,),
        in_specs=[rows, rows, anywhere, anywhere, anywhere],
        out_specs=[
            pl.BlockSpec((4, d, tile), lambda i: (0, 0, i)),
            pl.BlockSpec((d, ff // count), lambda i: (0, i)),
            anywhere,
            anywhere,
            anywhere,
        ],
        out_shape=[
            jax.ShapeDtypeStruct((4, d, tokens), BF),
            jax.ShapeDtypeStruct((d, ff), BF),
            jax.ShapeDtypeStruct((4, chunks, tokens // step, step, chunk), BF),
            jax.ShapeDtypeStruct((chunks, tokens // step, step, chunk), F32),
            jax.ShapeDtypeStruct((chunks, tokens // step, step, chunk), F32),
        ],
        scratch_shapes=[
            pltpu.VMEM(wg.shape, BF),
            pltpu.VMEM(wu.shape, BF),
            pltpu.VMEM(wd.shape, BF),
            pltpu.VMEM((4, chunks, high, step, chunk), BF),
            pltpu.VMEM((2, chunks, high, step, chunk), F32),
            pltpu.SemaphoreType.DMA((2, 3)),
            pltpu.SemaphoreType.DMA((chunks, 3)),
            pltpu.SemaphoreType.DMA((3,)),
        ],
        compiler_params=pltpu.CompilerParams(dimension_semantics=("arbitrary",), vmem_limit_bytes=VMEM_LIMIT),
    )(x, dy, wg, wu, wd)
    return outs[0], turned, *outs[1:], wdt


def sum_kernel(n, wide, turned, silu_1, slope_1, wdt, wg, wu, out, shard_a, shard_b, wide_1, *refs):
    g_ref, d_ref, i_ref, q_ref, go, own, left_op, right_op, wg_1, wu_1, wd_0, factors, thin, *sems = refs
    (op_sem, w_sem, tile_sem, stage_sem, out_sem, own_sem, d_s, d_r, i_s, i_r, ii_s, ii_r, iii_s, iii_r, ag1_s, ag1_r, ag2_s, ag2_r, p_s, p_r) = sems
    _, chunks, tiles, rows, chunk = wide.shape
    tokens, d = tiles * rows, turned.shape[1]
    mats, first = g_ref.shape[0], g_ref.shape[0] // 2
    early = go.shape[0]
    shards = (shard_a, shard_b)
    pieces = g_ref.shape[1]
    half = pieces // 2
    per = pieces // chunks
    lanes = g_ref.shape[-1]
    me = lax.axis_index("dp")
    core = lax.rem(me, 2)
    chip = me // 2
    chips = n // 2
    partner = me + 1 - 2 * core
    chip_r = lax.rem(chip + 1, chips)
    chip_l = lax.rem(chip + chips - 1, chips)
    chip_o = lax.rem(chip + 2, chips)
    toward = (chip_r, chip_l)
    behind = (chip_l, chip_r)
    device = tuple(2 * c + core for c in toward)

    def piece(c, h):
        return core * half + 2 * c + h

    def remote(src, dst, s, r, to):
        return pltpu.make_async_remote_copy(src, dst, s, r, device_id={"dp": to}, device_id_type=MESH)

    def d_copy(k):
        return remote(g_ref.at[k, pl.ds((1 - core) * half, half)], d_ref.at[k], d_s.at[k], d_r.at[k], partner)

    def i_copy(k, e):
        return remote(g_ref.at[k, piece(chip_o, e)], i_ref.at[k, e], i_s.at[k, e], i_r.at[k, e], device[e])

    def ii_copy(k, e):
        return remote(g_ref.at[k, piece(toward[e], 1 - e)], q_ref.at[k, e, 1 - e], ii_s.at[k, e], ii_r.at[k, e], device[e])

    def iii_copy(k, e):
        return remote(i_ref.at[k, e], q_ref.at[k, e, e], iii_s.at[k, e], iii_r.at[k, e], device[e])

    def ag1_copy(k, e, c):
        span = go.at[k, pl.ds(piece(c, 0), 2)]
        return remote(span, span, ag1_s.at[k, e], ag1_r.at[k, e], device[e])

    def ag2_copy(k, e, c):
        span = go.at[k, piece(c, e)]
        return remote(span, span, ag2_s.at[k, e], ag2_r.at[k, e], device[e])

    def p_copy(k, j, c, owner):
        span = go.at[k, pl.ds(owner * half + 2 * c, 2)]
        return remote(span, span, p_s.at[k, j], p_r.at[k, j], partner)

    def left_load(k, slot):
        return pltpu.make_async_copy(turned.at[(2 * k + 1) // 3], left_op.at[slot], op_sem.at[slot])

    def right_copy(t, later):
        k, c = t // chunks, lax.rem(t, chunks)
        c = lax.rem(c + (1 - core) * (chunks // 2), chunks)
        slot = lax.rem(t, 3)
        return pltpu.make_async_copy(wide_1.at[k - first - 1, c] if later else wide.at[k, c], right_op.at[slot], op_sem.at[2 + slot])

    def right_load(t):
        @pl.when(t < (first + 1) * chunks)
        def _():
            right_copy(t, False).start()

        @pl.when(t >= (first + 1) * chunks)
        def _():
            right_copy(t, True).start()

    weights = [
        pltpu.make_async_copy(wg.at[1], wg_1, w_sem.at[0]),
        pltpu.make_async_copy(wu.at[1], wu_1, w_sem.at[1]),
        pltpu.make_async_copy(wdt, wd_0, w_sem.at[2]),
    ]

    def tile_loads(i):
        odd = lax.rem(i, 2)
        span = pl.ds(pl.multiple_of(i * rows, rows), rows)
        half_slot = pl.ds(odd * chunks, chunks)
        pairs = [
            (wide.at[1, :, i], right_op.at[0, half_slot]),
            (wide.at[2, :, i], right_op.at[1, half_slot]),
            (silu_1.at[:, i], factors.at[0, odd]),
            (slope_1.at[:, i], factors.at[1, odd]),
            (turned.at[0, :, span], thin.at[0, odd]),
            (turned.at[2, :, span], thin.at[1, odd]),
        ]
        return [pltpu.make_async_copy(x, y, tile_sem.at[odd, j]) for j, (x, y) in enumerate(pairs)]

    def stages(i):
        return [pltpu.make_async_copy(right_op.at[2, pl.ds(j * chunks, chunks)], wide_1.at[j, :, i], stage_sem.at[j]) for j in range(2)]

    barrier = pltpu.get_barrier_semaphore()
    for to in (*device, partner):
        pl.semaphore_signal(barrier, inc=1, device_id={"dp": to}, device_id_type=MESH)
    left_load(0, 0).start()
    right_load(0)
    right_load(1)
    for c in weights:
        c.start()
    pl.semaphore_wait(barrier, 3)

    def multiply(t):
        k, c = t // chunks, lax.rem(t, chunks)

        @pl.when((c == 0) & (k != first))
        def _():
            left_load(k, lax.rem(k, 2)).wait()

        @pl.when((c == 0) & (k + 1 != first) & (k + 1 < mats))
        def _():
            left_load(k + 1, lax.rem(k + 1, 2)).start()

        pltpu.make_async_copy(wide.at[0, 0], right_op.at[lax.rem(t, 3)], op_sem.at[2 + lax.rem(t, 3)]).wait()

        @pl.when((t + 2 < first * chunks) | ((t >= first * chunks) & (t + 2 < mats * chunks)))
        def _():
            right_load(t + 2)

        where = lax.rem(c + (1 - core) * (chunks // 2), chunks) * per
        a = left_op[lax.rem(k, 2)]
        block = dot(a, right_op[lax.rem(t, 3)].reshape(tokens, chunk)).astype(BF)
        for j in range(per):
            g_ref[k, where + j] = block[:, j * lanes : (j + 1) * lanes]

        @pl.when(c == chunks // 2 - 1)
        def _():
            d_copy(k).start()

    def tile_of_layer_0(i):
        odd = lax.rem(i, 2)
        for c in tile_loads(i):
            c.wait()

        @pl.when((i > 0) & (i + 1 < tiles))
        def _():
            for c in tile_loads(i + 1)[2:]:
                c.start()

        dag = dau = None
        for c in range(chunks):
            cols = pl.ds(c * chunk, chunk)
            tg = dot_t(wg_1[:, cols], right_op[0, odd * chunks + c])
            tu = dot_t(wu_1[:, cols], right_op[1, odd * chunks + c])
            dag = tg if dag is None else dag + tg
            dau = tu if dau is None else dau + tu

        @pl.when(i + 2 < tiles)
        def _():
            for c in tile_loads(i + 2)[:2]:
                c.start()

        @pl.when(i + 1 == tiles)
        def _():
            right_load(first * chunks)
            right_load(first * chunks + 1)

        da = (dag.astype(BF) + dau.astype(BF)).astype(F32)
        high = thin[1, odd].astype(F32)
        scale = lax.rsqrt(jnp.mean(high * high, 0, keepdims=True) + 1e-6)
        slope = jnp.sum(da * high, 0, keepdims=True)
        change = da * scale - high * (scale * scale * scale * slope * (1.0 / d))
        dh = thin[0, odd] + change.astype(BF)
        left_op[first % 2, :, pl.ds(pl.multiple_of(i * rows, rows), rows)] = dh
        dh = dh.T

        @pl.when(i > 0)
        def _():
            for c in stages(i - 1):
                c.wait()

        for c in range(chunks):
            dp = dot(dh, wd_0[:, c * chunk : (c + 1) * chunk]).astype(BF).astype(F32)
            right_op[2, c] = (dp * factors[1, odd, c]).astype(BF)
            right_op[2, chunks + c] = (dp * factors[0, odd, c]).astype(BF)
        for c in stages(i):
            c.start()

    def reduce_1(k):
        d_copy(k).wait_recv()
        for c in (chip_o, chip_r, chip_l, chip):
            for h in range(2):
                one = g_ref[k, piece(c, h)].astype(F32) + d_ref[k, 2 * c + h].astype(F32)
                g_ref[k, piece(c, h)] = one.astype(BF)
        for e in range(2):
            i_copy(k, e).start()
        for e in range(2):
            ii_copy(k, e).start()

    def reduce_2(k):
        for e in range(2):
            i_copy(k, e).wait_recv()
            one = g_ref[k, piece(toward[e], e)].astype(F32) + i_ref[k, e].astype(F32)
            i_ref[k, e] = one.astype(BF)
            iii_copy(k, e).start()

    def reduce_3(k):
        for e in range(2):
            ii_copy(k, e).wait_recv()
            iii_copy(k, e).wait_recv()

        def total(h):
            one = g_ref[k, piece(chip, h)].astype(F32) + q_ref[k, 0, h].astype(F32) + q_ref[k, 1, h].astype(F32)
            return one.astype(BF)

        @pl.when(k < early)
        def _():
            for h in range(2):
                go[k, piece(chip, h)] = total(h)
            for e in range(2):
                ag1_copy(k, e, chip).start()
            p_copy(k, 0, chip, core).start()

        @pl.when(k >= early)
        def _():
            for h in range(2):
                own[h, k - early] = total(h)
            for h in range(2):
                own_copy(k - early, h).start()

    def own_copy(k, h):
        return pltpu.make_async_copy(own.at[h, k], shards[h].at[k], own_sem.at[k, h])

    def gather_2(k):
        for e in range(2):
            ag1_copy(k, e, behind[e]).wait_recv()
            ag2_copy(k, e, behind[e]).start()
            p_copy(k, 1 + e, behind[e], core).start()

    def gather_3(k):
        for e in range(2):
            ag2_copy(k, e, chip_o).wait_recv()
        p_copy(k, 3, chip_o, core).start()

    def done_copy(k):
        return pltpu.make_async_copy(go.at[k], out.at[k], out_sem.at[k])

    def finish(k):
        for j, c in enumerate((chip, *behind, chip_o)):
            p_copy(k, j, c, 1 - core).wait_recv()
        done_copy(k).start()

    def last_chunk(t):
        return lax.rem(t, chunks) == chunks - 1

    def first_half(t, carry):
        multiply(t)
        k = t // chunks

        @pl.when(last_chunk(t))
        def _():
            reduce_1(k)

            @pl.when(k > 0)
            def _():
                reduce_2(k - 1)

        return carry

    def middle(i, carry):
        tile_of_layer_0(i)

        @pl.when(i == 1)
        def _():
            reduce_2(first - 1)
            reduce_3(0)

        @pl.when(i == 4)
        def _():
            reduce_3(1)

        @pl.when(i == 5)
        def _():
            reduce_3(2)

        @pl.when(i == 6)
        def _():
            gather_2(0)

        return carry

    def second_half(t, carry):
        multiply(t)
        k = t // chunks

        @pl.when(last_chunk(t))
        def _():
            reduce_1(k)

            if early > 1:

                @pl.when(k == first)
                def _():
                    gather_2(1)

            @pl.when(k > first)
            def _():
                reduce_2(k - 1)

        return carry

    lax.fori_loop(0, first * chunks, first_half, 0)
    for c in weights:
        c.wait()
    for c in (*tile_loads(0), *tile_loads(1)):
        c.start()
    lax.fori_loop(0, tiles, middle, 0)
    for c in stages(tiles - 1):
        c.wait()
    lax.fori_loop(first * chunks, mats * chunks, second_half, 0)
    reduce_2(mats - 1)
    lax.fori_loop(first, mats - 1, lambda k, _: reduce_3(k), None)
    lax.fori_loop(0, early, lambda k, _: gather_3(k), None)
    lax.fori_loop(0, early, lambda k, _: finish(k), None)
    reduce_3(mats - 1)

    def drain(k, carry):
        d_copy(k).wait_send()
        for e in range(2):
            i_copy(k, e).wait_send()
            ii_copy(k, e).wait_send()
            iii_copy(k, e).wait_send()
        return carry

    def drain_early(k, carry):
        for e in range(2):
            ag1_copy(k, e, chip).wait_send()
            ag2_copy(k, e, behind[e]).wait_send()
        for j, c in enumerate((chip, *behind, chip_o)):
            p_copy(k, j, c, core).wait_send()
        done_copy(k).wait()
        return carry

    def drain_late(k, carry):
        for h in range(2):
            own_copy(k, h).wait()
        return carry

    lax.fori_loop(0, mats, drain, 0)
    lax.fori_loop(0, early, drain_early, 0)
    lax.fori_loop(0, mats - early, drain_late, 0)


def gradients(wide, turned, silu_1, slope_1, wdt, weights, n, early=2):
    _, chunks, tiles, rows, chunk = wide.shape
    d, tokens = turned.shape[1:]
    mats = 6
    late = mats - early
    pieces = 2 * n
    lanes = chunks * chunk // pieces
    dma = lambda *shape: pltpu.SemaphoreType.DMA(shape)
    return pl.pallas_call(
        functools.partial(sum_kernel, n),
        name="gradients",
        in_specs=[pl.BlockSpec(memory_space=pl.ANY)] * 7,
        out_specs=[pl.BlockSpec(memory_space=pl.ANY)] * 4,
        out_shape=[
            jax.ShapeDtypeStruct((early, pieces, d, lanes), BF),
            jax.ShapeDtypeStruct((late, d, lanes), BF),
            jax.ShapeDtypeStruct((late, d, lanes), BF),
            jax.ShapeDtypeStruct((2, chunks, tiles, rows, chunk), BF),
        ],
        scratch_shapes=[
            pltpu.VMEM((mats, pieces, d, lanes), BF),
            pltpu.VMEM((mats, pieces // 2, d, lanes), BF),
            pltpu.VMEM((mats, 2, d, lanes), BF),
            pltpu.VMEM((mats, 2, 2, d, lanes), BF),
            pltpu.VMEM((early, pieces, d, lanes), BF),
            pltpu.VMEM((2, late, d, lanes), BF),
            pltpu.VMEM((2, d, tokens), BF),
            pltpu.VMEM((3, tiles, rows, chunk), BF),
            pltpu.VMEM(weights[0].shape[1:], BF),
            pltpu.VMEM(weights[1].shape[1:], BF),
            pltpu.VMEM(wdt.shape, BF),
            pltpu.VMEM((2, 2, chunks, rows, chunk), F32),
            pltpu.VMEM((2, 2, d, rows), BF),
            dma(5),
            dma(3),
            dma(2, 6),
            dma(2),
            dma(early),
            dma(late, 2),
            dma(mats),
            dma(mats),
            *[dma(mats, 2)] * 6,
            *[dma(early, 2)] * 4,
            *[dma(early, 4)] * 2,
        ],
        compiler_params=pltpu.CompilerParams(collective_id=0, has_side_effects=True, vmem_limit_bytes=VMEM_LIMIT),
    )(wide, turned, silu_1, slope_1, wdt, *weights[:2])[:3]


def adamw(w, m, v, g):
    m = 0.9 * m + 0.1 * g
    v = 0.95 * v + 0.05 * g * g
    step = m * lax.rsqrt(v + 1e-8) + 0.1 * w
    return (w - 0.02 * step).astype(BF), m, v


def update_kernel(n, jobs, given, slots, *refs):
    sources, ins, outs = refs[:given], refs[given : given + 9], refs[-19:-10]
    bufs, in_sem, out_sem = refs[-10:-2], refs[-2], refs[-1]
    me = lax.axis_index("dp")
    chips = n // 2
    lanes = sources[0].shape[-1]
    width = 2 * lanes

    def shards(job):
        _, _, mat, s, where = job
        if isinstance(where, int):
            return [sources[s].at[mat, 2 * where + h] for h in range(2)]
        return [sources[s + h].at[mat] for h in range(2)]

    def spot(i):
        a, layer, _, _, where = jobs[i]
        tall = a == 2
        slot = len([1 for job in jobs[:i] if (job[0] == 2) == tall]) % slots
        if isinstance(where, int):
            block = where
        else:
            block = lax.rem(lax.rem(me, 2) + where[0], 2) * chips + lax.rem(me // 2 + where[1], chips)
        span = pl.ds(pl.multiple_of(block * width, width), width)
        at = (layer, span) if tall else (layer, slice(None), span)
        return at, slot + slots * tall, [b.at[slot] for b in bufs[4 * tall : 4 * tall + 4]]

    def loads(i):
        a = jobs[i][0]
        at, slot, (g, *held) = spot(i)
        pairs = [(ins[a + 3 * k].at[at], held[k]) for k in range(3)] + [(x, g.at[h]) for h, x in enumerate(shards(jobs[i]))]
        return [pltpu.make_async_copy(x, y, in_sem.at[5 * slot + k]) for k, (x, y) in enumerate(pairs)]

    def stores(i):
        a = jobs[i][0]
        at, slot, (_, *held) = spot(i)
        return [pltpu.make_async_copy(held[k], outs[a + 3 * k].at[at], out_sem.at[3 * slot + k]) for k in range(3)]

    def before(i):
        tall = jobs[i][0] == 2
        same = [k for k in range(i) if (jobs[k][0] == 2) == tall]
        return same[-slots] if len(same) >= slots else None

    def start(i):
        k = before(i)
        if k is not None:
            for c in stores(k):
                c.wait()
        for c in loads(i):
            c.start()

    ahead = slots // 2 + 2
    for i in range(min(ahead, len(jobs))):
        start(i)
    for i, (a, *_) in enumerate(jobs):
        if i + ahead < len(jobs):
            start(i + ahead)
        g, w, m, v = spot(i)[2]
        for c in loads(i):
            c.wait()
        if a == 2:
            count = w.shape[1] // lanes

            def rows(t, _):
                h, q = t // count, lax.rem(t, count)
                cols = pl.ds(pl.multiple_of(q * lanes, lanes), lanes)
                at = (pl.ds(pl.multiple_of(h * lanes, lanes), lanes), cols)
                w[at], m[at], v[at] = adamw(w[at].astype(F32), m[at], v[at], g[h, cols].astype(F32).T)

            lax.fori_loop(0, 2 * count, rows, None)
        else:
            high = 64

            def rows(t, _):
                span = pl.ds(pl.multiple_of(t * high, high), high)
                for h in range(2):
                    at = (span, pl.ds(h * lanes, lanes))
                    w[at], m[at], v[at] = adamw(w[at].astype(F32), m[at], v[at], g[h, span].astype(F32))

            lax.fori_loop(0, w.shape[0] // high, rows, None)
        for c in stores(i):
            c.start()
    for i in range(len(jobs)):
        if all(before(k) != i for k in range(len(jobs))):
            for c in stores(i):
                c.wait()


def update(n, whole, pairs, places, kinds_of, arrays, new=()):
    _, d, ff = arrays[0].shape
    width = ff // n
    sources = [*whole, *[x for pair in pairs for x in pair]]
    count = len(kinds_of) - pairs[0][0].shape[0]
    jobs = [(*kinds_of[k], k, 0, s) for s in range(n) for k in range(count)] if whole else []
    jobs += [(*kinds, k, len(whole) + 2 * s, place) for s, place in enumerate(places) for k, kinds in enumerate(kinds_of[count:])]
    depth = 8
    kinds = (BF, BF, F32, F32)
    held = [pltpu.VMEM((depth, *shape), kind) for low in ((d, width), (width, d)) for kind, shape in zip(kinds, ((2, d, width // 2), low, low, low))]
    given = len(sources)
    elements = len(jobs) * d * width
    return pl.pallas_call(
        functools.partial(update_kernel, n, jobs, given, depth),
        name="update",
        in_specs=[pl.BlockSpec(memory_space=pl.ANY)] * (given + 9 + len(new)),
        out_specs=[pl.BlockSpec(memory_space=pl.ANY)] * 9,
        out_shape=[jax.ShapeDtypeStruct(x.shape, x.dtype) for x in arrays],
        input_output_aliases={given + 9 + i: i for i in range(len(new))},
        scratch_shapes=[*held, pltpu.SemaphoreType.DMA((10 * depth,)), pltpu.SemaphoreType.DMA((6 * depth,))],
        cost_estimate=pl.CostEstimate(flops=150 * elements, bytes_accessed=22 * elements, transcendentals=elements),
        compiler_params=pltpu.CompilerParams(vmem_limit_bytes=VMEM_LIMIT),
    )(*sources, *arrays, *new)


def solution(mesh):
    n = mesh.shape["dp"]
    chips = n // 2
    to_right = [(i, (i + 2) % n) for i in range(n)]
    to_left = [(i, (i - 2) % n) for i in range(n)]
    across = [(i, i ^ 1) for i in range(n)]
    kinds_of = [(a, layer) for layer in (1, 0) for a in (2, 0, 1)]

    def send(pair, to):
        return tuple(lax.ppermute(x, "dp", to) for x in pair)

    def step(x, dy, *arrays):
        weights = arrays[:3]
        operands = chain(x[0], dy[0], *weights)
        g, *own = gradients(*operands, weights, n)
        left, right, other = send(own, to_right), send(own, to_left), send(own, across)
        new = update(n, [g], [own, other], [(0, 0), (1, 0)], kinds_of, arrays)
        left, right, first = lax.optimization_barrier((left, right, new[0]))
        new = [first, *new[1:]]
        far = (*send(left[:1], to_right), *send(right[1:], to_left))
        other_left, other_right = send(left, across), send(right, across)
        new = update(n, [], [left, right], [(0, chips - 1), (0, 1)], kinds_of, arrays, new)
        far, first = lax.optimization_barrier((far, new[0]))
        new = [first, *new[1:]]
        other_far = send(far, across)
        new = update(n, [], [other_left, other_right, far], [(1, chips - 1), (1, 1), (0, 2)], kinds_of, arrays, new)
        return tuple(update(n, [], [other_far], [(1, 2)], kinds_of, arrays, new))

    return jax.shard_map(
        step,
        mesh=mesh,
        in_specs=(P(("rep", "dp"), None, None),) * 2 + (P(None, None, None),) * 9,
        out_specs=(P("rep", None, None),) * 9,
        check_vma=False,
    )
```

```python
import functools

import jax
import jax.numpy as jnp
from jax import lax
from jax.experimental import pallas as pl
from jax.experimental.pallas import tpu as pltpu
from jax.sharding import PartitionSpec as P

BF, F32 = jnp.bfloat16, jnp.float32
MESH = pl.DeviceIdType.MESH
VMEM_LIMIT = 64 * 1024 * 1024 - 256 * 1024


def dot(a, b):
    return lax.dot_general(a, b, (((1,), (0,)), ((), ())), preferred_element_type=F32)


def dot_t(a, b):
    return lax.dot_general(a, b, (((1,), (1,)), ((), ())), preferred_element_type=F32)


def norm(h):
    wide = h.astype(F32)
    scale = lax.rsqrt(jnp.mean(wide * wide, -1, keepdims=True) + 1e-6)
    return (wide * scale).astype(BF)


def chain_kernel(chunk, x_ref, dy_ref, wg_in, wu_in, wd_in, turned, wdt, wide, silu_1, slope_1, wg, wu, wd, held, factors, w_sem, o_sem, f_sem):
    i = pl.program_id(0)
    steps = pl.num_programs(0)
    dyt, a2t, h1t, a1t = (turned.at[j] for j in range(4))
    chunks = wg.shape[-1] // chunk
    shape = held.shape[2:]
    rows = shape[0]

    def weights(layer):
        return [pltpu.make_async_copy(x.at[layer], y.at[layer], w_sem.at[layer, j]) for j, (x, y) in enumerate(((wg_in, wg), (wu_in, wu), (wd_in, wd)))]

    def early_out(i):
        span = pl.ds(i * rows, rows)
        pairs = ((held.at[3], wide.at[3, :, span]), (factors.at[0], silu_1.at[:, span]), (factors.at[1], slope_1.at[:, span]))
        return [pltpu.make_async_copy(x, y, f_sem.at[j]) for j, (x, y) in enumerate(pairs)]

    def late_out(i, c):
        return [pltpu.make_async_copy(held.at[j, c], wide.at[j, c, pl.ds(i * rows, rows)], o_sem.at[c, j]) for j in range(3)]

    @pl.when(i == 0)
    def _():
        for layer in range(2):
            for w in weights(layer):
                w.start()
        for w in weights(0):
            w.wait()

    @pl.when(i > 0)
    def _():
        for out in early_out(i - 1):
            out.wait()

    x = x_ref[...]
    a1 = norm(x)
    a1t[...] = a1.T
    down = None
    group = 2
    parts = [(j, slice(j * chunk, (j + 1) * chunk)) for j in range(group)]
    for c in range(0, chunks, group):
        cols = pl.ds(c * chunk, group * chunk)
        g = dot(a1, wg[0, :, cols])
        u = dot(a1, wu[0, :, cols])
        s = jax.nn.sigmoid(g)
        silu = g * s
        p = (silu * u).astype(BF)
        slope = u * (s * (1.0 + g * (1.0 - s)))
        for j, part in parts:
            held[3, c + j] = p[:, part].reshape(shape)
            factors[0, c + j] = silu[:, part].reshape(shape)
            factors[1, c + j] = slope[:, part].reshape(shape)
        term = dot(p, wd[0, cols, :])
        down = term if down is None else down + term
    h1 = x + down.astype(BF)
    h1t[...] = h1.T
    a2 = norm(h1)
    a2t[...] = a2.T
    dy = dy_ref[...]
    dyt[...] = dy.T
    turn = wdt.shape[-1]
    wdt[...] = wd[0, pl.ds(pl.multiple_of(i * turn, turn), turn), :].T
    for out in early_out(i):
        out.start()

    @pl.when(i == 0)
    def _():
        for w in weights(1):
            w.wait()

    @pl.when(i > 0)
    def _():
        for c in range(chunks):
            for out in late_out(i - 1, c):
                out.wait()

    for c in range(0, chunks, group):
        cols = pl.ds(c * chunk, group * chunk)
        g = dot(a2, wg[1, :, cols])
        u = dot(a2, wu[1, :, cols])
        dp = dot_t(dy, wd[1, cols, :]).astype(BF).astype(F32)
        s = jax.nn.sigmoid(g)
        silu = g * s
        p = (silu * u).astype(BF)
        du = (dp * silu).astype(BF)
        dg = (dp * (u * (s * (1.0 + g * (1.0 - s))))).astype(BF)
        for j, part in parts:
            held[0, c + j] = p[:, part].reshape(shape)
            held[2, c + j] = du[:, part].reshape(shape)
            held[1, c + j] = dg[:, part].reshape(shape)
        for j in range(group):
            for out in late_out(i, c + j):
                out.start()

    @pl.when(i == steps - 1)
    def _():
        for out in early_out(i):
            out.wait()
        for c in range(chunks):
            for out in late_out(i, c):
                out.wait()


def chain(x, dy, wg, wu, wd, tile=512, chunk=512, step=256):
    tokens, d = x.shape
    ff = wg.shape[-1]
    chunks, count, high = ff // chunk, tokens // tile, tile // step
    anywhere = pl.BlockSpec(memory_space=pl.ANY)
    rows = pl.BlockSpec((tile, d), lambda i: (i, 0))
    turned, wdt, *outs = pl.pallas_call(
        functools.partial(chain_kernel, chunk),
        name="chain",
        grid=(count,),
        in_specs=[rows, rows, anywhere, anywhere, anywhere],
        out_specs=[
            pl.BlockSpec((4, d, tile), lambda i: (0, 0, i)),
            pl.BlockSpec((d, ff // count), lambda i: (0, i)),
            anywhere,
            anywhere,
            anywhere,
        ],
        out_shape=[
            jax.ShapeDtypeStruct((4, d, tokens), BF),
            jax.ShapeDtypeStruct((d, ff), BF),
            jax.ShapeDtypeStruct((4, chunks, tokens // step, step, chunk), BF),
            jax.ShapeDtypeStruct((chunks, tokens // step, step, chunk), F32),
            jax.ShapeDtypeStruct((chunks, tokens // step, step, chunk), F32),
        ],
        scratch_shapes=[
            pltpu.VMEM(wg.shape, BF),
            pltpu.VMEM(wu.shape, BF),
            pltpu.VMEM(wd.shape, BF),
            pltpu.VMEM((4, chunks, high, step, chunk), BF),
            pltpu.VMEM((2, chunks, high, step, chunk), F32),
            pltpu.SemaphoreType.DMA((2, 3)),
            pltpu.SemaphoreType.DMA((chunks, 3)),
            pltpu.SemaphoreType.DMA((3,)),
        ],
        compiler_params=pltpu.CompilerParams(dimension_semantics=("arbitrary",), vmem_limit_bytes=VMEM_LIMIT),
    )(x, dy, wg, wu, wd)
    return outs[0], turned, *outs[1:], wdt


def sum_kernel(n, wide, turned, silu_1, slope_1, wdt, wg, wu, out, shard_a, shard_b, wide_1, *refs):
    g_ref, d_ref, i_ref, q_ref, go, own, left_op, right_op, wg_1, wu_1, wd_0, factors, thin, *sems = refs
    (op_sem, w_sem, tile_sem, stage_sem, out_sem, own_sem, d_s, d_r, i_s, i_r, ii_s, ii_r, iii_s, iii_r, ag1_s, ag1_r, ag2_s, ag2_r, p_s, p_r) = sems
    _, chunks, tiles, rows, chunk = wide.shape
    tokens, d = tiles * rows, turned.shape[1]
    mats, first = g_ref.shape[0], g_ref.shape[0] // 2
    early = go.shape[0]
    shards = (shard_a, shard_b)
    pieces = g_ref.shape[1]
    half = pieces // 2
    per = pieces // chunks
    lanes = g_ref.shape[-1]
    me = lax.axis_index("dp")
    core = lax.rem(me, 2)
    chip = me // 2
    chips = n // 2
    partner = me + 1 - 2 * core
    chip_r = lax.rem(chip + 1, chips)
    chip_l = lax.rem(chip + chips - 1, chips)
    chip_o = lax.rem(chip + 2, chips)
    toward = (chip_r, chip_l)
    behind = (chip_l, chip_r)
    device = tuple(2 * c + core for c in toward)

    def piece(c, h):
        return core * half + 2 * c + h

    def remote(src, dst, s, r, to):
        return pltpu.make_async_remote_copy(src, dst, s, r, device_id={"dp": to}, device_id_type=MESH)

    def d_copy(k):
        return remote(g_ref.at[k, pl.ds((1 - core) * half, half)], d_ref.at[k], d_s.at[k], d_r.at[k], partner)

    def i_copy(k, e):
        return remote(g_ref.at[k, piece(chip_o, e)], i_ref.at[k, e], i_s.at[k, e], i_r.at[k, e], device[e])

    def ii_copy(k, e):
        return remote(g_ref.at[k, piece(toward[e], 1 - e)], q_ref.at[k, e, 1 - e], ii_s.at[k, e], ii_r.at[k, e], device[e])

    def iii_copy(k, e):
        return remote(i_ref.at[k, e], q_ref.at[k, e, e], iii_s.at[k, e], iii_r.at[k, e], device[e])

    def ag1_copy(k, e, c):
        span = go.at[k, pl.ds(piece(c, 0), 2)]
        return remote(span, span, ag1_s.at[k, e], ag1_r.at[k, e], device[e])

    def ag2_copy(k, e, c):
        span = go.at[k, piece(c, e)]
        return remote(span, span, ag2_s.at[k, e], ag2_r.at[k, e], device[e])

    def p_copy(k, j, c, owner):
        span = go.at[k, pl.ds(owner * half + 2 * c, 2)]
        return remote(span, span, p_s.at[k, j], p_r.at[k, j], partner)

    def left_load(k, slot):
        return pltpu.make_async_copy(turned.at[(2 * k + 1) // 3], left_op.at[slot], op_sem.at[slot])

    def right_copy(t, later):
        k, c = t // chunks, lax.rem(t, chunks)
        c = lax.rem(c + (1 - core) * (chunks // 2), chunks)
        slot = lax.rem(t, 3)
        return pltpu.make_async_copy(wide_1.at[k - first - 1, c] if later else wide.at[k, c], right_op.at[slot], op_sem.at[2 + slot])

    def right_load(t):
        @pl.when(t < (first + 1) * chunks)
        def _():
            right_copy(t, False).start()

        @pl.when(t >= (first + 1) * chunks)
        def _():
            right_copy(t, True).start()

    weights = [
        pltpu.make_async_copy(wg.at[1], wg_1, w_sem.at[0]),
        pltpu.make_async_copy(wu.at[1], wu_1, w_sem.at[1]),
        pltpu.make_async_copy(wdt, wd_0, w_sem.at[2]),
    ]

    def tile_loads(i):
        odd = lax.rem(i, 2)
        span = pl.ds(pl.multiple_of(i * rows, rows), rows)
        half_slot = pl.ds(odd * chunks, chunks)
        pairs = [
            (wide.at[1, :, i], right_op.at[0, half_slot]),
            (wide.at[2, :, i], right_op.at[1, half_slot]),
            (silu_1.at[:, i], factors.at[0, odd]),
            (slope_1.at[:, i], factors.at[1, odd]),
            (turned.at[0, :, span], thin.at[0, odd]),
            (turned.at[2, :, span], thin.at[1, odd]),
        ]
        return [pltpu.make_async_copy(x, y, tile_sem.at[odd, j]) for j, (x, y) in enumerate(pairs)]

    def stages(i):
        return [pltpu.make_async_copy(right_op.at[2, pl.ds(j * chunks, chunks)], wide_1.at[j, :, i], stage_sem.at[j]) for j in range(2)]

    barrier = pltpu.get_barrier_semaphore()
    for to in (*device, partner):
        pl.semaphore_signal(barrier, inc=1, device_id={"dp": to}, device_id_type=MESH)
    left_load(0, 0).start()
    right_load(0)
    right_load(1)
    for c in weights:
        c.start()
    pl.semaphore_wait(barrier, 3)

    def multiply(t):
        k, c = t // chunks, lax.rem(t, chunks)

        @pl.when((c == 0) & (k != first))
        def _():
            left_load(k, lax.rem(k, 2)).wait()

        @pl.when((c == 0) & (k + 1 != first) & (k + 1 < mats))
        def _():
            left_load(k + 1, lax.rem(k + 1, 2)).start()

        pltpu.make_async_copy(wide.at[0, 0], right_op.at[lax.rem(t, 3)], op_sem.at[2 + lax.rem(t, 3)]).wait()

        @pl.when((t + 2 < first * chunks) | ((t >= first * chunks) & (t + 2 < mats * chunks)))
        def _():
            right_load(t + 2)

        where = lax.rem(c + (1 - core) * (chunks // 2), chunks) * per
        a = left_op[lax.rem(k, 2)]
        block = dot(a, right_op[lax.rem(t, 3)].reshape(tokens, chunk)).astype(BF)
        for j in range(per):
            g_ref[k, where + j] = block[:, j * lanes : (j + 1) * lanes]

        @pl.when(c == chunks // 2 - 1)
        def _():
            d_copy(k).start()

    def tile_of_layer_0(i):
        odd = lax.rem(i, 2)
        for c in tile_loads(i):
            c.wait()

        @pl.when((i > 0) & (i + 1 < tiles))
        def _():
            for c in tile_loads(i + 1)[2:]:
                c.start()

        dag = dau = None
        for c in range(chunks):
            cols = pl.ds(c * chunk, chunk)
            tg = dot_t(wg_1[:, cols], right_op[0, odd * chunks + c])
            tu = dot_t(wu_1[:, cols], right_op[1, odd * chunks + c])
            dag = tg if dag is None else dag + tg
            dau = tu if dau is None else dau + tu

        @pl.when(i + 2 < tiles)
        def _():
            for c in tile_loads(i + 2)[:2]:
                c.start()

        @pl.when(i + 1 == tiles)
        def _():
            right_load(first * chunks)
            right_load(first * chunks + 1)

        da = (dag.astype(BF) + dau.astype(BF)).astype(F32)
        high = thin[1, odd].astype(F32)
        scale = lax.rsqrt(jnp.mean(high * high, 0, keepdims=True) + 1e-6)
        slope = jnp.sum(da * high, 0, keepdims=True)
        change = da * scale - high * (scale * scale * scale * slope * (1.0 / d))
        dh = thin[0, odd] + change.astype(BF)
        left_op[first % 2, :, pl.ds(pl.multiple_of(i * rows, rows), rows)] = dh
        dh = dh.T

        @pl.when(i > 0)
        def _():
            for c in stages(i - 1):
                c.wait()

        for c in range(chunks):
            dp = dot(dh, wd_0[:, c * chunk : (c + 1) * chunk]).astype(BF).astype(F32)
            right_op[2, c] = (dp * factors[1, odd, c]).astype(BF)
            right_op[2, chunks + c] = (dp * factors[0, odd, c]).astype(BF)
        for c in stages(i):
            c.start()

    def reduce_1(k):
        d_copy(k).wait_recv()
        for j, c in enumerate((chip_o, chip_r, chip_l, chip)):
            for h in range(2):
                one = g_ref[k, piece(c, h)].astype(F32) + d_ref[k, 2 * c + h].astype(F32)
                g_ref[k, piece(c, h)] = one.astype(BF)
            if j == 1:
                for e in range(2):
                    i_copy(k, e).start()
        for e in range(2):
            ii_copy(k, e).start()

    def reduce_2(k):
        for e in range(2):
            i_copy(k, e).wait_recv()
            one = g_ref[k, piece(toward[e], e)].astype(F32) + i_ref[k, e].astype(F32)
            i_ref[k, e] = one.astype(BF)
            iii_copy(k, e).start()

    def reduce_3(k):
        for e in range(2):
            ii_copy(k, e).wait_recv()
            iii_copy(k, e).wait_recv()

        def total(h):
            one = g_ref[k, piece(chip, h)].astype(F32) + q_ref[k, 0, h].astype(F32) + q_ref[k, 1, h].astype(F32)
            return one.astype(BF)

        @pl.when(k < early)
        def _():
            for h in range(2):
                go[k, piece(chip, h)] = total(h)
            for e in range(2):
                ag1_copy(k, e, chip).start()
            p_copy(k, 0, chip, core).start()

        @pl.when(k >= early)
        def _():
            for h in range(2):
                own[h, k - early] = total(h)
            for h in range(2):
                own_copy(k - early, h).start()

    def own_copy(k, h):
        return pltpu.make_async_copy(own.at[h, k], shards[h].at[k], own_sem.at[k, h])

    def gather_2(k):
        for e in range(2):
            ag1_copy(k, e, behind[e]).wait_recv()
            ag2_copy(k, e, behind[e]).start()
            p_copy(k, 1 + e, behind[e], core).start()

    def gather_3(k):
        for e in range(2):
            ag2_copy(k, e, chip_o).wait_recv()
        p_copy(k, 3, chip_o, core).start()

    def done_copy(k):
        return pltpu.make_async_copy(go.at[k], out.at[k], out_sem.at[k])

    def finish(k):
        for j, c in enumerate((chip, *behind, chip_o)):
            p_copy(k, j, c, 1 - core).wait_recv()
        done_copy(k).start()

    def last_chunk(t):
        return lax.rem(t, chunks) == chunks - 1

    def first_half(t, carry):
        multiply(t)
        k = t // chunks

        @pl.when(last_chunk(t))
        def _():
            reduce_1(k)

            @pl.when(k > 0)
            def _():
                reduce_2(k - 1)

        return carry

    def middle(i, carry):
        tile_of_layer_0(i)

        @pl.when(i == 1)
        def _():
            reduce_2(first - 1)
            reduce_3(0)

        @pl.when(i == 4)
        def _():
            reduce_3(1)

        @pl.when(i == 6)
        def _():
            gather_2(0)

        return carry

    def second_half(t, carry):
        multiply(t)
        k = t // chunks

        @pl.when(last_chunk(t))
        def _():
            reduce_1(k)

            if early > 1:

                @pl.when(k == first)
                def _():
                    gather_2(1)

            @pl.when(k > first)
            def _():
                reduce_2(k - 1)

        return carry

    lax.fori_loop(0, first * chunks, first_half, 0)
    for c in weights:
        c.wait()
    for c in (*tile_loads(0), *tile_loads(1)):
        c.start()
    lax.fori_loop(0, tiles, middle, 0)
    for c in stages(tiles - 1):
        c.wait()
    lax.fori_loop(first * chunks, mats * chunks, second_half, 0)
    reduce_2(mats - 1)
    lax.fori_loop(first - 1, mats - 1, lambda k, _: reduce_3(k), None)
    lax.fori_loop(0, early, lambda k, _: gather_3(k), None)
    lax.fori_loop(0, early, lambda k, _: finish(k), None)
    reduce_3(mats - 1)

    def drain(k, carry):
        d_copy(k).wait_send()
        for e in range(2):
            i_copy(k, e).wait_send()
            ii_copy(k, e).wait_send()
            iii_copy(k, e).wait_send()
        return carry

    def drain_early(k, carry):
        for e in range(2):
            ag1_copy(k, e, chip).wait_send()
            ag2_copy(k, e, behind[e]).wait_send()
        for j, c in enumerate((chip, *behind, chip_o)):
            p_copy(k, j, c, core).wait_send()
        done_copy(k).wait()
        return carry

    def drain_late(k, carry):
        for h in range(2):
            own_copy(k, h).wait()
        return carry

    lax.fori_loop(0, mats, drain, 0)
    lax.fori_loop(0, early, drain_early, 0)
    lax.fori_loop(0, mats - early, drain_late, 0)


def gradients(wide, turned, silu_1, slope_1, wdt, weights, n, early=2):
    _, chunks, tiles, rows, chunk = wide.shape
    d, tokens = turned.shape[1:]
    mats = 6
    late = mats - early
    pieces = 2 * n
    lanes = chunks * chunk // pieces
    dma = lambda *shape: pltpu.SemaphoreType.DMA(shape)
    return pl.pallas_call(
        functools.partial(sum_kernel, n),
        name="gradients",
        in_specs=[pl.BlockSpec(memory_space=pl.ANY)] * 7,
        out_specs=[pl.BlockSpec(memory_space=pl.ANY)] * 4,
        out_shape=[
            jax.ShapeDtypeStruct((early, pieces, d, lanes), BF),
            jax.ShapeDtypeStruct((late, d, lanes), BF),
            jax.ShapeDtypeStruct((late, d, lanes), BF),
            jax.ShapeDtypeStruct((2, chunks, tiles, rows, chunk), BF),
        ],
        scratch_shapes=[
            pltpu.VMEM((mats, pieces, d, lanes), BF),
            pltpu.VMEM((mats, pieces // 2, d, lanes), BF),
            pltpu.VMEM((mats, 2, d, lanes), BF),
            pltpu.VMEM((mats, 2, 2, d, lanes), BF),
            pltpu.VMEM((early, pieces, d, lanes), BF),
            pltpu.VMEM((2, late, d, lanes), BF),
            pltpu.VMEM((2, d, tokens), BF),
            pltpu.VMEM((3, tiles, rows, chunk), BF),
            pltpu.VMEM(weights[0].shape[1:], BF),
            pltpu.VMEM(weights[1].shape[1:], BF),
            pltpu.VMEM(wdt.shape, BF),
            pltpu.VMEM((2, 2, chunks, rows, chunk), F32),
            pltpu.VMEM((2, 2, d, rows), BF),
            dma(5),
            dma(3),
            dma(2, 6),
            dma(2),
            dma(early),
            dma(late, 2),
            dma(mats),
            dma(mats),
            *[dma(mats, 2)] * 6,
            *[dma(early, 2)] * 4,
            *[dma(early, 4)] * 2,
        ],
        compiler_params=pltpu.CompilerParams(collective_id=0, has_side_effects=True, vmem_limit_bytes=VMEM_LIMIT),
    )(wide, turned, silu_1, slope_1, wdt, *weights[:2])[:3]


def adamw(w, m, v, g):
    m = 0.9 * m + 0.1 * g
    v = 0.95 * v + 0.05 * g * g
    step = m * lax.rsqrt(v + 1e-8) + 0.1 * w
    return (w - 0.02 * step).astype(BF), m, v


def update_kernel(n, jobs, given, slots, *refs):
    sources, ins, outs = refs[:given], refs[given : given + 9], refs[-19:-10]
    bufs, in_sem, out_sem = refs[-10:-2], refs[-2], refs[-1]
    me = lax.axis_index("dp")
    chips = n // 2
    lanes = sources[0].shape[-1]
    width = 2 * lanes

    def shards(job):
        _, _, mat, s, where = job
        if isinstance(where, int):
            return [sources[s].at[mat, 2 * where + h] for h in range(2)]
        return [sources[s + h].at[mat] for h in range(2)]

    def spot(i):
        a, layer, _, _, where = jobs[i]
        tall = a == 2
        slot = len([1 for job in jobs[:i] if (job[0] == 2) == tall]) % slots
        if isinstance(where, int):
            block = where
        else:
            block = lax.rem(lax.rem(me, 2) + where[0], 2) * chips + lax.rem(me // 2 + where[1], chips)
        span = pl.ds(pl.multiple_of(block * width, width), width)
        at = (layer, span) if tall else (layer, slice(None), span)
        return at, slot + slots * tall, [b.at[slot] for b in bufs[4 * tall : 4 * tall + 4]]

    def loads(i):
        a = jobs[i][0]
        at, slot, (g, *held) = spot(i)
        pairs = [(ins[a + 3 * k].at[at], held[k]) for k in range(3)] + [(x, g.at[h]) for h, x in enumerate(shards(jobs[i]))]
        return [pltpu.make_async_copy(x, y, in_sem.at[5 * slot + k]) for k, (x, y) in enumerate(pairs)]

    def stores(i):
        a = jobs[i][0]
        at, slot, (_, *held) = spot(i)
        return [pltpu.make_async_copy(held[k], outs[a + 3 * k].at[at], out_sem.at[3 * slot + k]) for k in range(3)]

    def before(i):
        tall = jobs[i][0] == 2
        same = [k for k in range(i) if (jobs[k][0] == 2) == tall]
        return same[-slots] if len(same) >= slots else None

    def start(i):
        k = before(i)
        if k is not None:
            for c in stores(k):
                c.wait()
        for c in loads(i):
            c.start()

    ahead = slots // 2 + 2
    for i in range(min(ahead, len(jobs))):
        start(i)
    for i, (a, *_) in enumerate(jobs):
        if i + ahead < len(jobs):
            start(i + ahead)
        g, w, m, v = spot(i)[2]
        for c in loads(i):
            c.wait()
        if a == 2:
            count = w.shape[1] // lanes

            def rows(t, _):
                h, q = t // count, lax.rem(t, count)
                cols = pl.ds(pl.multiple_of(q * lanes, lanes), lanes)
                at = (pl.ds(pl.multiple_of(h * lanes, lanes), lanes), cols)
                w[at], m[at], v[at] = adamw(w[at].astype(F32), m[at], v[at], g[h, cols].astype(F32).T)

            lax.fori_loop(0, 2 * count, rows, None)
        else:
            high = 64

            def rows(t, _):
                span = pl.ds(pl.multiple_of(t * high, high), high)
                for h in range(2):
                    at = (span, pl.ds(h * lanes, lanes))
                    w[at], m[at], v[at] = adamw(w[at].astype(F32), m[at], v[at], g[h, span].astype(F32))

            lax.fori_loop(0, w.shape[0] // high, rows, None)
        for c in stores(i):
            c.start()
    for i in range(len(jobs)):
        if all(before(k) != i for k in range(len(jobs))):
            for c in stores(i):
                c.wait()


def update(n, whole, pairs, places, kinds_of, arrays, new=()):
    _, d, ff = arrays[0].shape
    width = ff // n
    sources = [*whole, *[x for pair in pairs for x in pair]]
    count = len(kinds_of) - pairs[0][0].shape[0]
    jobs = [(*kinds_of[k], k, 0, s) for s in range(n) for k in range(count)] if whole else []
    jobs += [(*kinds, k, len(whole) + 2 * s, place) for s, place in enumerate(places) for k, kinds in enumerate(kinds_of[count:])]
    depth = 8
    kinds = (BF, BF, F32, F32)
    held = [pltpu.VMEM((depth, *shape), kind) for low in ((d, width), (width, d)) for kind, shape in zip(kinds, ((2, d, width // 2), low, low, low))]
    given = len(sources)
    elements = len(jobs) * d * width
    return pl.pallas_call(
        functools.partial(update_kernel, n, jobs, given, depth),
        name="update",
        in_specs=[pl.BlockSpec(memory_space=pl.ANY)] * (given + 9 + len(new)),
        out_specs=[pl.BlockSpec(memory_space=pl.ANY)] * 9,
        out_shape=[jax.ShapeDtypeStruct(x.shape, x.dtype) for x in arrays],
        input_output_aliases={given + 9 + i: i for i in range(len(new))},
        scratch_shapes=[*held, pltpu.SemaphoreType.DMA((10 * depth,)), pltpu.SemaphoreType.DMA((6 * depth,))],
        cost_estimate=pl.CostEstimate(flops=150 * elements, bytes_accessed=22 * elements, transcendentals=elements),
        compiler_params=pltpu.CompilerParams(vmem_limit_bytes=VMEM_LIMIT),
    )(*sources, *arrays, *new)


def solution(mesh):
    n = mesh.shape["dp"]
    chips = n // 2
    to_right = [(i, (i + 2) % n) for i in range(n)]
    to_left = [(i, (i - 2) % n) for i in range(n)]
    across = [(i, i ^ 1) for i in range(n)]
    kinds_of = [(a, layer) for layer in (1, 0) for a in (2, 0, 1)]

    def send(pair, to):
        return tuple(lax.ppermute(x, "dp", to) for x in pair)

    def step(x, dy, *arrays):
        weights = arrays[:3]
        operands = chain(x[0], dy[0], *weights)
        g, *own = gradients(*operands, weights, n)
        left, right, other = send(own, to_right), send(own, to_left), send(own, across)
        new = update(n, [g], [own, other], [(0, 0), (1, 0)], kinds_of, arrays)
        left, right, first = lax.optimization_barrier((left, right, new[0]))
        new = [first, *new[1:]]
        far = (*send(left[:1], to_right), *send(right[1:], to_left))
        other_left, other_right = send(left, across), send(right, across)
        new = update(n, [], [left, right], [(0, chips - 1), (0, 1)], kinds_of, arrays, new)
        far, first = lax.optimization_barrier((far, new[0]))
        new = [first, *new[1:]]
        other_far = send(far, across)
        new = update(n, [], [other_left, other_right, far], [(1, chips - 1), (1, 1), (0, 2)], kinds_of, arrays, new)
        return tuple(update(n, [], [other_far], [(1, 2)], kinds_of, arrays, new))

    return jax.shard_map(
        step,
        mesh=mesh,
        in_specs=(P(("rep", "dp"), None, None),) * 2 + (P(None, None, None),) * 9,
        out_specs=(P("rep", None, None),) * 9,
        check_vma=False,
    )
```
